32 devices in a mesh: dom: 16 (over z, y, x), sub: 2 (over core).
Axes of the slice: x: 2, y: 2, z: 4, core: 2. Of those that a mesh axis runs over, the one named last changes fastest.
Arguments:
- rhs: float32 [8192], P(('dom', 'sub')), may hold values from -6 to 6
- diagonal: float32 [8192], P(('dom', 'sub')), may hold values from 1 to 2
- self_raw: float32 [8192, 256], P(('dom', 'sub')), may hold values from -0.046875 to 0.046875
- coupling: float32 [8192, 256], P(('dom', 'sub')), may hold values from -0.046875 to 0.046875
- pattern: int32 [64, 2], P(('dom', 'sub')), may hold values 0 or 1
- prolong: float32 [8192, 128], P(('dom', 'sub')), may hold values from -0.5 to 0.5
- coarse_raw: float32 [4096, 256], P('dom'), may hold values from -0.0234375 to 0.0234375
- coarse_diagonal: float32 [4096], P('dom'), may hold values from 1 to 2
Outputs:
- solution: float32 [8192], P(('dom', 'sub'))
- residual: float32 [8192], P(('dom', 'sub'))
- norms: float32 [3], replicated
The draws below stay inside these ranges and needn't reach their ends.
All inputs are finite; a program needn't handle non-finite values. No bound on the sum of `pattern` on one device may be relied on, other than what follows from the above.
Results may differ from the reference program's by a relative error of at most 0.0003.
Values sent between devices are 32-bit elements; how exact they have to be, the bound alone decides.
A program may use at most 64 MiB of HBM per device.

```python
import jax
import jax.numpy as jnp
from jax import lax

B = 128
NB = 2
NC = 128
ITERS = 3
DEVS = 32
ROWS = 8192
N_DOM = 16
N_SUB = 2


def place_ends(array, key, low, top_value):
    extent = array.shape
    place = [jax.random.randint(jax.random.fold_in(key, axis), (), 0, extent[axis]) for axis in range(len(extent))]
    array = array.at[tuple(place)].set(low)
    longest = extent.index(max(extent))
    place[longest] = (place[longest] + 1) % extent[longest]
    return array.at[tuple(place)].set(top_value)


def block_levels(own_key, dims, split, least, high):
    loudness, own = 1.0, jax.random.fold_in(own_key, 6)
    for axis_at, shards_of in split:
        heights = jnp.exp(jax.random.uniform(jax.random.fold_in(own, axis_at), (shards_of,), jnp.float32, least / len(split), high / len(split)))
        loudness = loudness * jnp.repeat(heights, dims[axis_at] // shards_of).reshape([-1 if axis == axis_at else 1 for axis in range(len(dims))])
    return loudness


def centred(key, shape, scale, limit, cuts=(), kind=jnp.bfloat16):
    values = scale * jax.random.normal(key, shape, jnp.float32)
    if cuts:
        values = values * block_levels(key, shape, cuts, -0.22, 0.18)
    return jnp.clip(values, -limit, limit).astype(kind)


def setup_inputs(seed: int = 0) -> dict:
    arg_keys = jax.random.split(jax.random.key(seed), 9)
    return {
        "rhs": centred(arg_keys[0], (ROWS,), 1.0, 6.0, ((0, 32),), jnp.float32),
        "diagonal": jnp.clip(1.0 + 1.0 * jax.random.uniform(arg_keys[1], (ROWS,), jnp.float32) ** block_levels(arg_keys[1], (ROWS,), ((0, 32),), -0.2, 0.2), 1.0, 2.0),
        "self_raw": centred(arg_keys[2], (ROWS, NB * B), (NB * B * NB * B // 4) ** -0.5, 0.046875, ((0, 32),), jnp.float32),
        "coupling": centred(arg_keys[3], (ROWS, NB * B), (NB * B * NB * B // 4) ** -0.5, 0.046875, ((0, 32),), jnp.float32),
        "pattern": place_ends((jax.random.randint(arg_keys[4], (DEVS * NB, NB), 0, 3) < 2).astype(jnp.int32), jax.random.fold_in(arg_keys[4], 1), 0, 1),
        "prolong": centred(arg_keys[5], (ROWS, NC), NC ** -0.5, 0.5, ((0, 32),), jnp.float32),
        "coarse_raw": centred(arg_keys[6], (N_DOM * 2 * NC, 2 * NC), (4 * NC * NC) ** -0.5, 0.0234375, ((0, 16),), jnp.float32),
        "coarse_diagonal": jnp.clip(1.0 + 1.0 * jax.random.uniform(arg_keys[7], (N_DOM * 2 * NC,), jnp.float32) ** block_levels(arg_keys[7], (N_DOM * 2 * NC,), ((0, 16),), -0.2, 0.2), 1.0, 2.0),
    }


OMEGA = 0.7
HIGH = lax.Precision.HIGHEST


def reference(rhs, diagonal, self_raw, coupling, pattern, prolong, coarse_raw, coarse_diagonal):
    devs = N_DOM * N_SUB
    width = NB * B
    chips = N_DOM
    eye = jnp.eye(width, dtype=jnp.float32)
    raw = self_raw.reshape(devs, width, width)
    diag = diagonal.reshape(devs, width)
    selfm = 0.5 * (raw + jnp.transpose(raw, (0, 2, 1))) * (1.0 - eye) + eye * diag[:, :, None]
    mask = pattern.reshape(devs, NB, 1, NB, 1).astype(jnp.float32)
    mask = jnp.broadcast_to(mask, (devs, NB, B, NB, B)).reshape(devs, width, width)
    coup = coupling.reshape(devs, width, width) * mask
    dinv = 1.0 / diag
    pro = prolong.reshape(devs, width, NC)
    ceye = jnp.eye(2 * NC, dtype=jnp.float32)
    craw = coarse_raw.reshape(chips, 2 * NC, 2 * NC)
    cdiag = coarse_diagonal.reshape(chips, 2 * NC)
    cmat = 0.5 * (craw + jnp.transpose(craw, (0, 2, 1))) * (1.0 - ceye) + ceye * cdiag[:, :, None]
    cdinv = 1.0 / cdiag
    zero_row = jnp.zeros((1, width), jnp.float32)

    def apply(vec):
        own = jnp.einsum('dij,dj->di', selfm, vec, precision=HIGH)
        nxt = jnp.concatenate([vec[1:], zero_row], axis=0)
        upper = jnp.einsum('dij,dj->di', coup, nxt, precision=HIGH)
        low = jnp.einsum('dji,dj->di', coup, vec, precision=HIGH)
        low = jnp.concatenate([zero_row, low[:-1]], axis=0)
        return own + upper + low

    def precond(wvec):
        first = OMEGA * dinv * wvec
        resid = wvec - apply(first)
        rcoarse = jnp.einsum('dij,di->dj', pro, resid, precision=HIGH).reshape(chips, 2 * NC)
        eone = cdinv * rcoarse
        etwo = eone + cdinv * (rcoarse - jnp.einsum('cij,cj->ci', cmat, eone, precision=HIGH))
        second = first + jnp.einsum('dij,dj->di', pro, etwo.reshape(devs, NC), precision=HIGH)
        return second + OMEGA * dinv * (wvec - apply(second))

    resid = rhs.reshape(devs, width)
    solution = jnp.zeros_like(resid)
    uvec = precond(resid)
    wvec = apply(uvec)
    zeros = jnp.zeros_like(resid)
    pvec, svec, qvec, zvec = zeros, zeros, zeros, zeros
    gamma_prev = jnp.float32(1.0)
    alpha_prev = jnp.float32(1.0)
    norm_list = []
    for step in range(ITERS):
        gamma = jnp.sum(resid * uvec)
        delta = jnp.sum(wvec * uvec)
        norm_list.append(jnp.sum(resid * resid))
        mvec = precond(wvec)
        nvec = apply(mvec)
        if step == 0:
            beta = jnp.float32(0.0)
            alpha = gamma / delta
        else:
            beta = gamma / gamma_prev
            alpha = gamma / (delta - beta * gamma / alpha_prev)
        zvec = nvec + beta * zvec
        qvec = mvec + beta * qvec
        svec = wvec + beta * svec
        pvec = uvec + beta * pvec
        solution = solution + alpha * pvec
        resid = resid - alpha * svec
        uvec = uvec - alpha * qvec
        wvec = wvec - alpha * zvec
        gamma_prev = gamma
        alpha_prev = alpha
    return solution.reshape(-1), resid.reshape(-1), jnp.stack(norm_list)
```

```python
import functools

import jax
import jax.numpy as jnp
from jax import lax
from jax.experimental import pallas as pl
from jax.experimental.pallas import tpu as pltpu
from jax.sharding import PartitionSpec as P

ITERS = 3
OMEGA = 0.7
MESH = pl.DeviceIdType.MESH
LANES = 128


def factor(count):
    side = 1
    for trial in range(1, count + 1):
        if trial * trial <= count and count % trial == 0:
            side = trial
    return count // side, side


def fold(matrix, row):
    total = None
    for start in range(0, matrix.shape[1], LANES):
        part = matrix[:, start : start + LANES] * row[:, start : start + LANES]
        total = part if total is None else total + part
    return total


def lanes(block):
    return jnp.sum(block, axis=1, keepdims=True)


def down(matrix, column):
    return jnp.sum(matrix * column, axis=0, keepdims=True)


def eye_of():
    rows = lax.broadcasted_iota(jnp.int32, (LANES, LANES), 0)
    cols = lax.broadcasted_iota(jnp.int32, (LANES, LANES), 1)
    return rows == cols


def embed(row):
    eye = eye_of()
    parts = [
        jnp.where(eye, row[:, start : start + LANES], 0.0) for start in range(0, row.shape[1], LANES)
    ]
    return jnp.concatenate(parts, axis=0)


def upright(row):
    return lanes(embed(row))


def flat(column):
    eye = eye_of()
    parts = [
        jnp.sum(jnp.where(eye, column[start : start + LANES], 0.0), axis=0, keepdims=True)
        for start in range(0, column.shape[0], LANES)
    ]
    return jnp.concatenate(parts, axis=1)


def kernel(
    n_dom, n_sub,
    rhs_ref, diag_ref, self_ref, coup_ref, pat_ref, pro_ref, craw_ref, cdiag_ref,
    sol_ref, res_ref, norm_ref,
    lines, s_raw, c_raw, p_raw, k_raw, kdiag, own_lines,
    f_mat, ft_mat, g_mat, t_mat, pt_mat, k_mat,
    up_out, low_out, up_in, low_in, snd_a, snd_b, next_buf, prev_buf,
    part_buf, red_buf, pack_out, pack_in,
    known, load_sem, line_send, line_recv, mat_send, mat_recv, edge_send, edge_recv,
    a_send, b_send, next_recv, prev_recv, r_send, r_recv, pack_send, pack_recv,
):
    dom, sub = lax.axis_index("dom"), lax.axis_index("sub")
    width = rhs_ref.shape[1]
    blocks = pat_ref.shape[0]
    brow = width // blocks
    coarse = pro_ref.shape[1]
    has_prev, has_next = dom > 0, dom < n_dom - 1
    n_row, n_col = factor(n_dom)
    barrier = pltpu.get_barrier_semaphore()
    last = ITERS - 1
    lane = lax.broadcasted_iota(jnp.int32, (1, LANES), 1)

    def remote(source, target, send, recv, device):
        return pltpu.make_async_remote_copy(
            source, target, send, recv, device_id=device, device_id_type=MESH
        )

    def line_copy():
        return remote(lines, lines, line_send, line_recv, (dom, 1))

    def mat_copy(index):
        source = (self_ref, coup_ref, pro_ref)[index]
        target = (s_raw, c_raw, p_raw)[index].at[0]
        return remote(source, target, mat_send.at[index], mat_recv.at[index], (dom, 1))

    def pack_copy():
        return remote(pack_out, pack_in, pack_send, pack_recv, (dom, 0))

    def finish(scalars, step, gamma_prev, alpha_prev):
        gamma, delta = scalars[:, 0:1], scalars[:, 1:2]
        if step == 0:
            return gamma, jnp.zeros_like(gamma), gamma / delta
        beta = gamma / gamma_prev
        return gamma, beta, gamma / (delta - beta * gamma / alpha_prev)

    def put_norms(norm_list):
        place_of = lax.broadcasted_iota(jnp.int32, norm_ref.shape, 1)
        norms = jnp.zeros(norm_ref.shape, jnp.float32)
        for step in range(ITERS):
            norms = jnp.where(place_of == step, norm_list[step], norms)
        norm_ref[...] = norms

    @pl.when(sub == 0)
    def _():
        loads = [
            pltpu.make_async_copy(source, lines.at[index], load_sem.at[index])
            for index, source in enumerate([rhs_ref, diag_ref])
        ]
        for load in loads:
            load.start()
        place = lax.broadcasted_iota(jnp.int32, (1, width), 1)
        for i in range(blocks):
            mask = jnp.zeros((1, width), jnp.float32)
            for j in range(blocks):
                mask = jnp.where(place // brow == j, pat_ref[i, j].astype(jnp.float32), mask)
            lines[2 + i] = mask
        pl.semaphore_wait(barrier, 1)
        for load in loads:
            load.wait()
        line_copy().start()
        for index in range(3):
            mat_copy(index).start()
        line_copy().wait_send()
        for index in range(3):
            mat_copy(index).wait_send()
        pack_copy().wait_recv()
        sol, resid, uvec, wvec, pvec, svec = [pack_in[index : index + 1] for index in range(6)]
        misc = pack_in[6:7]
        every = red_buf.at[last]
        pltpu.make_async_copy(every, every, r_recv.at[last]).wait()
        total = jnp.sum(red_buf[last], axis=0)
        gamma, beta, alpha = finish(total, last, misc[:, 0:1], misc[:, 1:2])
        sol_ref[...] = sol + alpha * (uvec + beta * pvec)
        res_ref[...] = resid - alpha * (wvec + beta * svec)
        put_norms([misc[:, 2 + step : 3 + step] for step in range(last)] + [total[:, 2:3]])

    @pl.when(sub == 1)
    def _():
        row_at, col_at = dom // n_col, dom % n_col
        pl.semaphore_signal(barrier, inc=1, device_id=(dom, 0), device_id_type=MESH)

        @pl.when(has_prev)
        def _():
            pl.semaphore_signal(barrier, inc=1, device_id=(dom - 1, 1), device_id_type=MESH)

        @pl.when(has_next)
        def _():
            pl.semaphore_signal(barrier, inc=1, device_id=(dom + 1, 1), device_id_type=MESH)

        def in_row(step):
            return (row_at * n_col + (col_at + step) % n_col, 1)

        def in_col(step):
            return (((row_at + step) % n_row) * n_col + col_at, 1)

        if n_col > 1:
            @pl.loop(1, n_col)
            def _(step):
                pl.semaphore_signal(barrier, inc=1, device_id=in_row(step), device_id_type=MESH)

        @pl.loop(1, n_row)
        def _(step):
            pl.semaphore_signal(barrier, inc=1, device_id=in_col(step), device_id_type=MESH)

        loads = [
            pltpu.make_async_copy(source, target, load_sem.at[index])
            for index, (source, target) in enumerate([
                (rhs_ref, own_lines.at[0]), (diag_ref, own_lines.at[1]), (coup_ref, c_raw.at[1]),
                (self_ref, s_raw.at[1]), (pro_ref, p_raw.at[1]), (craw_ref, k_raw), (cdiag_ref, kdiag),
            ])
        ]
        for load in loads:
            load.start()

        @pl.when(dom == 0)
        def _():
            low_in[...] = jnp.zeros_like(low_in)
            prev_buf[...] = jnp.zeros_like(prev_buf)
            g_mat[...] = jnp.zeros_like(g_mat)

        @pl.when(dom == n_dom - 1)
        def _():
            up_in[...] = jnp.zeros_like(up_in)
            next_buf[...] = jnp.zeros_like(next_buf)

        def first_up():
            return remote(up_out, up_in, edge_send.at[0], edge_recv.at[0], (dom - 1, 1))

        def first_low():
            return remote(low_out, low_in, edge_send.at[1], edge_recv.at[1], (dom + 1, 1))

        def edge_matrix():
            return remote(ft_mat, g_mat, edge_send.at[2], edge_recv.at[2], (dom + 1, 1))

        def to_prev(k):
            return remote(snd_a.at[k], next_buf.at[k], a_send.at[k], next_recv.at[k], (dom - 1, 1))

        def to_next(k):
            return remote(snd_b.at[k], prev_buf.at[k], b_send.at[k], prev_recv.at[k], (dom + 1, 1))

        def send(k, vec):
            snd_a[k] = vec[:, :width]
            snd_b[k] = vec[:, width:]

            @pl.when(has_prev)
            def _():
                to_prev(k).start()

            @pl.when(has_next)
            def _():
                to_next(k).start()

        def receive(k):
            @pl.when(has_prev)
            def _():
                to_next(k).wait_recv()

            @pl.when(has_next)
            def _():
                to_prev(k).wait_recv()

        for load in loads[:3]:
            load.wait()
        for i in range(blocks):
            for j in range(blocks):
                at = (slice(i * brow, (i + 1) * brow), slice(j * brow, (j + 1) * brow))
                f_mat[at] = c_raw[1, at[0], at[1]] * pat_ref[i, j].astype(jnp.float32)
        ft_mat[...] = f_mat[...].T
        rhs_b, diag_b = own_lines[0], own_lines[1]
        scale_b = OMEGA * (1.0 / diag_b)
        first_b = scale_b * rhs_b
        low_out[0] = down(f_mat[...], upright(first_b))
        low_out[1] = scale_b

        pl.semaphore_wait(
            barrier,
            (n_row - 1) + (n_col - 1) + has_prev.astype(jnp.int32) + has_next.astype(jnp.int32),
        )

        @pl.loop(1, n_row)
        def _(step):
            pl.semaphore_signal(known, inc=1, device_id=in_col(step), device_id_type=MESH)

        @pl.when(has_next)
        def _():
            first_low().start()

        line_copy().wait_recv()
        rhs_a, diag_a = lines[0], lines[1]
        scale_a = OMEGA * (1.0 / diag_a)
        first_a = scale_a * rhs_a
        up_out[0] = first_a
        up_out[1] = scale_a

        @pl.when(has_prev)
        def _():
            first_up().start()

        @pl.when(has_next)
        def _():
            edge_matrix().start()

        rows = lax.broadcasted_iota(jnp.int32, (width, width), 0)
        cols = lax.broadcasted_iota(jnp.int32, (width, width), 1)
        same = rows == cols

        def put_self(index, diag):
            raw = s_raw[index]
            at = slice(index * width, (index + 1) * width)
            t_mat[at, at] = jnp.where(same, diag - diag * (1.0 / OMEGA), 0.5 * (raw + raw.T))

        for load in loads[3:]:
            load.wait()
        put_self(1, diag_b)
        pt_mat[1] = p_raw[1].T
        kinv = 1.0 / kdiag[...]
        craw = k_raw[...]
        k_mat[...] = jnp.where(same, -kinv, (0.5 * (craw + craw.T)) * kinv * upright(kinv))

        rhs = jnp.concatenate([rhs_a, rhs_b], axis=1)
        scale = jnp.concatenate([scale_a, scale_b], axis=1)
        heavy = jnp.concatenate([diag_a, diag_b], axis=1) * (1.0 / OMEGA)
        minus = -upright(scale)

        mat_copy(0).wait_recv()
        put_self(0, diag_a)
        mat_copy(1).wait_recv()
        for i in range(blocks):
            at = slice(i * brow, (i + 1) * brow)
            block = c_raw[0, at, :] * lines[2 + i]
            t_mat[at, width:] = block
            t_mat[width:, at] = block.T
        mat_copy(2).wait_recv()
        pt_mat[0] = p_raw[0].T

        def start_sums(step, resid, uvec, wvec):
            gamma, delta, rnorm = lanes(resid * uvec), lanes(wvec * uvec), lanes(resid * resid)
            line = jnp.where(lane == 0, gamma, jnp.where(lane == 1, delta, rnorm))
            part_buf[step] = line
            red_buf[step, pl.ds(dom, 1)] = line[None]
            if step == 0:
                pl.semaphore_wait(known, n_row - 1)

            @pl.loop(1, n_dom)
            def _(offset):
                for other in range(n_sub) if step == last else (1,):
                    remote(
                        part_buf.at[step], red_buf.at[step, dom], r_send.at[step], r_recv.at[step],
                        ((dom + offset) % n_dom, other),
                    ).start()

            if step == last:
                remote(
                    part_buf.at[step], red_buf.at[step, dom], r_send.at[step], r_recv.at[step], (dom, 0)
                ).start()

        def end_sums(step):
            others = red_buf.at[step, pl.ds(0, n_dom - 1)]
            pltpu.make_async_copy(others, others, r_recv.at[step]).wait()
            return jnp.sum(red_buf[step], axis=0)

        def halves(block):
            return block[:width], block[width:]

        def round_of(t, vec, begin, middle):
            first = scale * vec
            if t:
                send(3 * t, first)
            begin()
            base = fold(t_mat[...], first)
            if t == 0:
                @pl.when(has_next)
                def _():
                    first_up().wait_recv()

                @pl.when(has_prev)
                def _():
                    first_low().wait_recv()

                edge_a, edge_b = embed(low_in[0]), fold(f_mat[...], up_in[0])
            else:
                receive(3 * t)
                edge_a, edge_b = fold(g_mat[...], prev_buf[3 * t]), fold(f_mat[...], next_buf[3 * t])
            base_a, base_b = halves(base)
            rough = jnp.concatenate(
                [down(p_raw[0], lanes(base_a + edge_a)), down(p_raw[1], lanes(base_b + edge_b))], axis=1
            )
            etwo = lanes(fold(k_mat[...], rough))
            second = first + jnp.concatenate(
                [down(pt_mat[0], etwo[:coarse]), down(pt_mat[1], etwo[coarse:])], axis=1
            )
            send(3 * t + 1, second)
            base = fold(t_mat[...], second) - embed(vec)
            send(3 * t + 2, -scale * flat(lanes(base)))
            side_next = jnp.where(has_next, up_in[1], 0.0)
            side_prev = jnp.where(has_prev, low_in[1], 0.0)
            upper = upright(second)
            on_next = side_next * down(f_mat[...], upper[width:])
            if t == 0:
                @pl.when(has_prev)
                def _():
                    edge_matrix().wait_recv()

            on_prev = side_prev * down(g_mat[...], upper[:width])
            extra = middle()
            receive(3 * t + 1)
            base_a, base_b = halves(base)
            col_a = minus[:width] * lanes(base_a + fold(g_mat[...], prev_buf[3 * t + 1]))
            col_b = minus[width:] * lanes(base_b + fold(f_mat[...], next_buf[3 * t + 1]))
            mvec = jnp.concatenate([flat(col_a), flat(col_b)], axis=1)
            own = down(t_mat[:width, :], col_a) + down(t_mat[width:, :], col_b) + heavy * mvec
            receive(3 * t + 2)
            edge = jnp.concatenate([
                flat(lanes(fold(g_mat[...], prev_buf[3 * t + 2] - on_prev))),
                flat(lanes(fold(f_mat[...], next_buf[3 * t + 2] - on_next))),
            ], axis=1)
            return mvec, own + edge, extra

        resid = rhs
        uvec, wvec, _ = round_of(0, resid, lambda: None, lambda: None)
        zeros = jnp.zeros_like(resid)
        pvec, svec, qvec, zvec, solution = (zeros,) * 5
        norm_list = []
        gamma = alpha = None
        for step in range(last):
            def begin():
                start_sums(step, resid, uvec, wvec)

            def middle():
                sums = end_sums(step)
                return sums, finish(sums, step, gamma, alpha)

            mvec, nvec, (total, (gamma, beta, alpha)) = round_of(step + 1, wvec, begin, middle)
            norm_list.append(total[:, 2:3])
            svec = wvec + beta * svec
            pvec = uvec + beta * pvec
            solution = solution + alpha * pvec
            resid = resid - alpha * svec
            zvec = nvec + beta * zvec
            qvec = mvec + beta * qvec
            uvec = uvec - alpha * qvec
            wvec = wvec - alpha * zvec
        start_sums(last, resid, uvec, wvec)
        for index, vec in enumerate([solution, resid, uvec, wvec, pvec, svec]):
            pack_out[index : index + 1] = vec[:, :width]
        misc = jnp.where(lane == 0, gamma, alpha)
        for step in range(last):
            misc = jnp.where(lane == 2 + step, norm_list[step], misc)
        pack_out[6:7, :LANES] = misc
        pack_copy().start()
        total = end_sums(last)
        gamma, beta, alpha = finish(total, last, gamma, alpha)
        sol_ref[...] = (solution + alpha * (uvec + beta * pvec))[:, width:]
        res_ref[...] = (resid - alpha * (wvec + beta * svec))[:, width:]
        put_norms(norm_list + [total[:, 2:3]])

        pack_copy().wait_send()

        @pl.when(has_prev)
        def _():
            first_up().wait_send()
            for k in range(1, 3 * ITERS):
                to_prev(k).wait_send()

        @pl.when(has_next)
        def _():
            first_low().wait_send()
            edge_matrix().wait_send()
            for k in range(1, 3 * ITERS):
                to_next(k).wait_send()

        for step in range(ITERS):
            sent = red_buf.at[step, pl.ds(0, n_dom - 1)]
            pltpu.make_async_copy(sent, sent, r_send.at[step]).wait()
            if step == last:
                every = red_buf.at[step]
                pltpu.make_async_copy(every, every, r_send.at[step]).wait()


def solution(mesh):
    n_dom, n_sub = mesh.shape["dom"], mesh.shape["sub"]

    def per_device(rhs, diagonal, self_raw, coupling, pattern, prolong, coarse_raw, coarse_diagonal):
        width = rhs.shape[0]
        coarse = prolong.shape[1]
        blocks = pattern.shape[0]
        steps = 3 * ITERS
        vmem = pl.BlockSpec(memory_space=pltpu.VMEM)
        smem = pl.BlockSpec(memory_space=pltpu.SMEM)
        hbm = pl.BlockSpec(memory_space=pl.ANY)
        single = jnp.float32
        dma = pltpu.SemaphoreType.DMA
        square = pltpu.VMEM((width, width), single)
        pair = pltpu.VMEM((2, 1, width), single)
        each = pltpu.VMEM((steps, 1, width), single)
        sol, res, norms = pl.pallas_call(
            functools.partial(kernel, n_dom, n_sub),
            out_shape=(
                jax.ShapeDtypeStruct((1, width), single),
                jax.ShapeDtypeStruct((1, width), single),
                jax.ShapeDtypeStruct((1, ITERS), single),
            ),
            in_specs=[hbm, hbm, hbm, hbm, smem, hbm, hbm, hbm],
            out_specs=(vmem, vmem, vmem),
            scratch_shapes=[
                pltpu.VMEM((2 + blocks, 1, width), single),
                pltpu.VMEM((2, width, width), single),
                pltpu.VMEM((2, width, width), single),
                pltpu.VMEM((2, width, coarse), single),
                pltpu.VMEM((2 * coarse, 2 * coarse), single),
                pltpu.VMEM((1, 2 * coarse), single),
                pair,
                square, square, square,
                pltpu.VMEM((2 * width, 2 * width), single),
                pltpu.VMEM((2, coarse, width), single),
                pltpu.VMEM((2 * coarse, 2 * coarse), single),
                pair, pair, pair, pair, each, each, each, each,
                pltpu.VMEM((ITERS, 1, LANES), single),
                pltpu.VMEM((ITERS, n_dom, 1, LANES), single),
                pltpu.VMEM((8, width), single),
                pltpu.VMEM((8, width), single),
                pltpu.SemaphoreType.REGULAR,
                dma((7,)), dma, dma, dma((3,)), dma((3,)), dma((3,)), dma((3,)),
                dma((steps,)), dma((steps,)), dma((steps,)), dma((steps,)),
                dma((ITERS,)), dma((ITERS,)), dma, dma,
            ],
            compiler_params=pltpu.CompilerParams(collective_id=0, has_side_effects=True),
        )(
            rhs.reshape(1, width), diagonal.reshape(1, width), self_raw, coupling, pattern,
            prolong, coarse_raw, coarse_diagonal.reshape(1, -1),
        )
        return sol.reshape(width), res.reshape(width), norms.reshape(ITERS)

    line = P(("dom", "sub"))
    table = P(("dom", "sub"), None)
    return jax.shard_map(
        per_device,
        mesh=mesh,
        in_specs=(line, line, table, table, table, table, P("dom", None), P("dom")),
        out_specs=(line, line, P()),
        check_vma=False,
    )
```

```python
import functools

import jax
import jax.numpy as jnp
from jax import lax
from jax.experimental import pallas as pl
from jax.experimental.pallas import tpu as pltpu
from jax.sharding import PartitionSpec as P

ITERS = 3
OMEGA = 0.7
MESH = pl.DeviceIdType.MESH
LANES = 128
GRANT = 56_516_000


def factor(count):
    side = 1
    for trial in range(1, count + 1):
        if trial * trial <= count and count % trial == 0:
            side = trial
    return count // side, side


def fold(matrix, row):
    total = None
    for start in range(0, matrix.shape[1], LANES):
        part = matrix[:, start : start + LANES] * row[:, start : start + LANES]
        total = part if total is None else total + part
    return total


def lanes(block):
    return jnp.sum(block, axis=1, keepdims=True)


def down(matrix, column):
    return jnp.sum(matrix * column, axis=0, keepdims=True)


def eye_of():
    rows = lax.broadcasted_iota(jnp.int32, (LANES, LANES), 0)
    cols = lax.broadcasted_iota(jnp.int32, (LANES, LANES), 1)
    return rows == cols


def embed(row):
    eye = eye_of()
    parts = [
        jnp.where(eye, row[:, start : start + LANES], 0.0) for start in range(0, row.shape[1], LANES)
    ]
    return jnp.concatenate(parts, axis=0)


def upright(row):
    return lanes(embed(row))


def flat(column):
    eye = eye_of()
    parts = [
        jnp.sum(jnp.where(eye, column[start : start + LANES], 0.0), axis=0, keepdims=True)
        for start in range(0, column.shape[0], LANES)
    ]
    return jnp.concatenate(parts, axis=1)


def kernel(
    n_dom, n_sub,
    rhs_ref, diag_ref, self_ref, coup_ref, pat_ref, pro_ref, craw_ref, cdiag_ref,
    out_ref,
    lines, s_raw, c_raw, p_raw, k_raw,
    f_mat, ft_mat, g_mat, t_mat, pt_mat, k_mat,
    up_out, low_out, up_in, low_in, snd_a, snd_b, next_buf, prev_buf,
    part_buf, red_buf, pack_out, pack_in,
    known, load_sem, line_send, line_recv, mat_send, mat_recv, edge_send, edge_recv,
    a_send, b_send, next_recv, prev_recv, r_send, r_recv, pack_send, pack_recv,
):
    dom, sub = lax.axis_index("dom"), lax.axis_index("sub")
    width = rhs_ref.shape[1]
    blocks = pat_ref.shape[0]
    brow = width // blocks
    coarse = pro_ref.shape[1]
    has_prev, has_next = dom > 0, dom < n_dom - 1
    n_row, n_col = factor(n_dom)
    barrier = pltpu.get_barrier_semaphore()
    last = ITERS - 1
    lane = lax.broadcasted_iota(jnp.int32, (1, LANES), 1)

    def remote(source, target, send, recv, device):
        return pltpu.make_async_remote_copy(
            source, target, send, recv, device_id=device, device_id_type=MESH
        )

    def line_copy():
        return remote(lines, lines, line_send, line_recv, (dom, 1))

    def mat_copy(index):
        source = (self_ref, coup_ref, pro_ref)[index]
        target = (s_raw, c_raw, p_raw)[index].at[0]
        return remote(source, target, mat_send.at[index], mat_recv.at[index], (dom, 1))

    def pack_copy():
        return remote(pack_out, pack_in, pack_send, pack_recv, (dom, 0))

    def finish(scalars, step, gamma_inv, alpha_inv):
        gamma, delta = scalars[:, 0:1], scalars[:, 1:2]
        if step == 0:
            return gamma, jnp.zeros_like(gamma), gamma / delta
        beta = gamma * gamma_inv
        return gamma, beta, gamma / (delta - beta * gamma * alpha_inv)

    def put(sol, res, norm_list):
        out_ref[0:1] = sol
        out_ref[1:2] = res
        place_of = lax.broadcasted_iota(jnp.int32, (1, width), 1)
        norms = jnp.zeros((1, width), jnp.float32)
        for step in range(ITERS):
            norms = jnp.where(place_of == step, norm_list[step], norms)
        out_ref[2:3] = norms

    @pl.when(sub == 0)
    def _():
        lines[0] = rhs_ref[...]
        lines[1] = diag_ref[...]
        place = lax.broadcasted_iota(jnp.int32, (1, width), 1)
        for i in range(blocks):
            mask = jnp.zeros((1, width), jnp.float32)
            for j in range(blocks):
                mask = jnp.where(place // brow == j, pat_ref[i : i + 1, j : j + 1].astype(jnp.float32), mask)
            lines[2 + i] = mask
        pl.semaphore_wait(barrier, 1)
        line_copy().start()
        for index in range(3):
            mat_copy(index).start()
        line_copy().wait_send()
        for index in range(3):
            mat_copy(index).wait_send()
        pack_copy().wait_recv()
        sol, resid, uvec, wvec, pvec, svec = [pack_in[index : index + 1] for index in range(6)]
        misc = pack_in[6:7]
        gamma_inv, alpha_inv = 1.0 / misc[:, 0:1], 1.0 / misc[:, 1:2]
        every = red_buf.at[last]
        pltpu.make_async_copy(every, every, r_recv.at[last]).wait()
        total = jnp.sum(red_buf[last], axis=0)
        gamma, beta, alpha = finish(total, last, gamma_inv, alpha_inv)
        put(
            sol + alpha * (uvec + beta * pvec),
            resid - alpha * (wvec + beta * svec),
            [misc[:, 2 + step : 3 + step] for step in range(last)] + [total[:, 2:3]],
        )

    @pl.when(sub == 1)
    def _():
        row_at, col_at = dom // n_col, dom % n_col
        pl.semaphore_signal(barrier, inc=1, device_id=(dom, 0), device_id_type=MESH)

        @pl.when(has_prev)
        def _():
            pl.semaphore_signal(barrier, inc=1, device_id=(dom - 1, 1), device_id_type=MESH)

        @pl.when(has_next)
        def _():
            pl.semaphore_signal(barrier, inc=1, device_id=(dom + 1, 1), device_id_type=MESH)

        def in_row(step):
            return (row_at * n_col + (col_at + step) % n_col, 1)

        def in_col(step):
            return (((row_at + step) % n_row) * n_col + col_at, 1)

        if n_col > 1:
            @pl.loop(1, n_col)
            def _(step):
                pl.semaphore_signal(barrier, inc=1, device_id=in_row(step), device_id_type=MESH)

        @pl.loop(1, n_row)
        def _(step):
            pl.semaphore_signal(barrier, inc=1, device_id=in_col(step), device_id_type=MESH)

        loads = [
            pltpu.make_async_copy(source, target, load_sem.at[index])
            for index, (source, target) in enumerate([
                (coup_ref, c_raw.at[1]), (self_ref, s_raw.at[1]), (pro_ref, p_raw.at[1]), (craw_ref, k_raw),
            ])
        ]
        for load in loads:
            load.start()

        @pl.when(dom == 0)
        def _():
            low_in[...] = jnp.zeros_like(low_in)
            prev_buf[...] = jnp.zeros_like(prev_buf)
            g_mat[...] = jnp.zeros_like(g_mat)

        @pl.when(dom == n_dom - 1)
        def _():
            up_in[...] = jnp.zeros_like(up_in)
            next_buf[...] = jnp.zeros_like(next_buf)

        def first_up():
            return remote(up_out, up_in, edge_send.at[0], edge_recv.at[0], (dom - 1, 1))

        def first_low():
            return remote(low_out, low_in, edge_send.at[1], edge_recv.at[1], (dom + 1, 1))

        def edge_matrix():
            return remote(ft_mat, g_mat, edge_send.at[2], edge_recv.at[2], (dom + 1, 1))

        def to_prev(k):
            return remote(snd_a.at[k], next_buf.at[k], a_send.at[k], next_recv.at[k], (dom - 1, 1))

        def to_next(k):
            return remote(snd_b.at[k], prev_buf.at[k], b_send.at[k], prev_recv.at[k], (dom + 1, 1))

        def send(k, vec):
            snd_a[k] = vec[:, :width]
            snd_b[k] = vec[:, width:]

            @pl.when(has_prev)
            def _():
                to_prev(k).start()

            @pl.when(has_next)
            def _():
                to_next(k).start()

        def receive(k):
            @pl.when(has_prev)
            def _():
                to_next(k).wait_recv()

            @pl.when(has_next)
            def _():
                to_prev(k).wait_recv()

        loads[0].wait()
        for i in range(blocks):
            for j in range(blocks):
                at = (slice(i * brow, (i + 1) * brow), slice(j * brow, (j + 1) * brow))
                f_mat[at] = c_raw[1, at[0], at[1]] * pat_ref[i : i + 1, j : j + 1].astype(jnp.float32)
        ft_mat[...] = f_mat[...].T
        rhs_b, diag_b = rhs_ref[...], diag_ref[...]
        scale_b = OMEGA * (1.0 / diag_b)
        first_b = scale_b * rhs_b
        low_out[0] = down(f_mat[...], upright(first_b))
        low_out[1] = scale_b

        pl.semaphore_wait(
            barrier,
            (n_row - 1) + (n_col - 1) + has_prev.astype(jnp.int32) + has_next.astype(jnp.int32),
        )

        @pl.loop(1, n_row)
        def _(step):
            pl.semaphore_signal(known, inc=1, device_id=in_col(step), device_id_type=MESH)

        @pl.when(has_next)
        def _():
            first_low().start()

        line_copy().wait_recv()
        rhs_a, diag_a = lines[0], lines[1]
        scale_a = OMEGA * (1.0 / diag_a)
        first_a = scale_a * rhs_a
        up_out[0] = first_a
        up_out[1] = scale_a

        @pl.when(has_prev)
        def _():
            first_up().start()

        @pl.when(has_next)
        def _():
            edge_matrix().start()

        rows = lax.broadcasted_iota(jnp.int32, (width, width), 0)
        cols = lax.broadcasted_iota(jnp.int32, (width, width), 1)
        same = rows == cols

        def put_self(index, diag):
            raw = s_raw[index]
            at = slice(index * width, (index + 1) * width)
            t_mat[at, at] = jnp.where(same, diag - diag * (1.0 / OMEGA), 0.5 * (raw + raw.T))

        for load in loads[1:]:
            load.wait()
        put_self(1, diag_b)
        pt_mat[1] = p_raw[1].T
        kinv = 1.0 / cdiag_ref[...]
        craw = k_raw[...]
        k_mat[...] = jnp.where(same, -kinv, (0.5 * (craw + craw.T)) * kinv * upright(kinv))

        rhs = jnp.concatenate([rhs_a, rhs_b], axis=1)
        scale = jnp.concatenate([scale_a, scale_b], axis=1)
        heavy = jnp.concatenate([diag_a, diag_b], axis=1) * (1.0 / OMEGA)
        minus = -upright(scale)

        mat_copy(0).wait_recv()
        put_self(0, diag_a)
        mat_copy(1).wait_recv()
        for i in range(blocks):
            at = slice(i * brow, (i + 1) * brow)
            block = c_raw[0, at, :] * lines[2 + i]
            t_mat[at, width:] = block
            t_mat[width:, at] = block.T
        mat_copy(2).wait_recv()
        pt_mat[0] = p_raw[0].T

        def start_sums(step, resid, uvec, wvec):
            gamma, delta, rnorm = lanes(resid * uvec), lanes(wvec * uvec), lanes(resid * resid)
            line = jnp.where(lane == 0, gamma, jnp.where(lane == 1, delta, rnorm))
            part_buf[step] = line
            red_buf[step, pl.ds(dom, 1)] = line[None]
            if step == 0:
                pl.semaphore_wait(known, n_row - 1)

            @pl.loop(0, n_dom - 1)
            def _(index):
                target = index + (index >= dom).astype(jnp.int32)
                for other in range(n_sub) if step == last else (1,):
                    remote(
                        part_buf.at[step], red_buf.at[step, dom], r_send.at[step], r_recv.at[step],
                        (target, other),
                    ).start()

            if step == last:
                remote(
                    part_buf.at[step], red_buf.at[step, dom], r_send.at[step], r_recv.at[step], (dom, 0)
                ).start()

        def end_sums(step):
            others = red_buf.at[step, pl.ds(0, n_dom - 1)]
            pltpu.make_async_copy(others, others, r_recv.at[step]).wait()
            return jnp.sum(red_buf[step], axis=0)

        def halves(block):
            return block[:width], block[width:]

        def round_of(t, vec, begin, middle):
            first = scale * vec
            if t:
                send(3 * t, first)
            begin()
            base = fold(t_mat[...], first)
            if t == 0:
                @pl.when(has_next)
                def _():
                    first_up().wait_recv()

                @pl.when(has_prev)
                def _():
                    first_low().wait_recv()

                edge_a, edge_b = embed(low_in[0]), fold(f_mat[...], up_in[0])
            else:
                receive(3 * t)
                edge_a, edge_b = fold(g_mat[...], prev_buf[3 * t]), fold(f_mat[...], next_buf[3 * t])
            base_a, base_b = halves(base)
            rough = jnp.concatenate(
                [down(p_raw[0], lanes(base_a + edge_a)), down(p_raw[1], lanes(base_b + edge_b))], axis=1
            )
            etwo = lanes(fold(k_mat[...], rough))
            second = first + jnp.concatenate(
                [down(pt_mat[0], etwo[:coarse]), down(pt_mat[1], etwo[coarse:])], axis=1
            )
            send(3 * t + 1, second)
            base = fold(t_mat[...], second) - embed(vec)
            send(3 * t + 2, -scale * flat(lanes(base)))
            side_next = jnp.where(has_next, up_in[1], 0.0)
            side_prev = jnp.where(has_prev, low_in[1], 0.0)
            upper = upright(second)
            on_next = side_next * down(f_mat[...], upper[width:])
            if t == 0:
                @pl.when(has_prev)
                def _():
                    edge_matrix().wait_recv()

            on_prev = side_prev * down(g_mat[...], upper[:width])
            extra = middle()
            receive(3 * t + 1)
            base_a, base_b = halves(base)
            col_a = minus[:width] * lanes(base_a + fold(g_mat[...], prev_buf[3 * t + 1]))
            col_b = minus[width:] * lanes(base_b + fold(f_mat[...], next_buf[3 * t + 1]))
            mvec = jnp.concatenate([flat(col_a), flat(col_b)], axis=1)
            own = down(t_mat[:width, :], col_a) + down(t_mat[width:, :], col_b) + heavy * mvec
            receive(3 * t + 2)
            edge = jnp.concatenate([
                flat(lanes(fold(g_mat[...], prev_buf[3 * t + 2] - on_prev))),
                flat(lanes(fold(f_mat[...], next_buf[3 * t + 2] - on_next))),
            ], axis=1)
            return mvec, own + edge, extra

        resid = rhs
        uvec, wvec, _ = round_of(0, resid, lambda: None, lambda: None)
        zeros = jnp.zeros_like(resid)
        pvec, svec, qvec, zvec, solution = (zeros,) * 5
        norm_list = []
        gamma_inv = alpha_inv = None
        for step in range(last):
            def begin():
                start_sums(step, resid, uvec, wvec)

            def middle():
                sums = end_sums(step)
                return sums, finish(sums, step, gamma_inv, alpha_inv)

            mvec, nvec, (total, (gamma, beta, alpha)) = round_of(step + 1, wvec, begin, middle)
            gamma_inv, alpha_inv = 1.0 / gamma, 1.0 / alpha
            norm_list.append(total[:, 2:3])
            svec = wvec + beta * svec
            pvec = uvec + beta * pvec
            solution = solution + alpha * pvec
            resid = resid - alpha * svec
            zvec = nvec + beta * zvec
            qvec = mvec + beta * qvec
            uvec = uvec - alpha * qvec
            wvec = wvec - alpha * zvec
        start_sums(last, resid, uvec, wvec)
        for index, vec in enumerate([solution, resid, uvec, wvec, pvec, svec]):
            pack_out[index : index + 1] = vec[:, :width]
        misc = jnp.where(lane == 0, gamma, alpha)
        for step in range(last):
            misc = jnp.where(lane == 2 + step, norm_list[step], misc)
        pack_out[6:7, :LANES] = misc
        pack_copy().start()
        total = end_sums(last)
        gamma, beta, alpha = finish(total, last, gamma_inv, alpha_inv)
        put(
            (solution + alpha * (uvec + beta * pvec))[:, width:],
            (resid - alpha * (wvec + beta * svec))[:, width:],
            norm_list + [total[:, 2:3]],
        )

        pack_copy().wait_send()

        @pl.when(has_prev)
        def _():
            first_up().wait_send()
            for k in range(1, 3 * ITERS):
                to_prev(k).wait_send()

        @pl.when(has_next)
        def _():
            first_low().wait_send()
            edge_matrix().wait_send()
            for k in range(1, 3 * ITERS):
                to_next(k).wait_send()

        for step in range(ITERS):
            sent = red_buf.at[step, pl.ds(0, n_dom - 1)]
            pltpu.make_async_copy(sent, sent, r_send.at[step]).wait()
            if step == last:
                every = red_buf.at[step]
                pltpu.make_async_copy(every, every, r_send.at[step]).wait()


def unpack(packed_ref, sol_ref, res_ref, norm_ref):
    sol_ref[...] = packed_ref[0]
    res_ref[...] = packed_ref[1]
    norm_ref[...] = packed_ref[2, : norm_ref.shape[0]]


def solution(mesh):
    n_dom, n_sub = mesh.shape["dom"], mesh.shape["sub"]

    def per_device(rhs, diagonal, self_raw, coupling, pattern, prolong, coarse_raw, coarse_diagonal):
        width = rhs.shape[0]
        coarse = prolong.shape[1]
        blocks = pattern.shape[0]
        steps = 3 * ITERS
        vmem = pl.BlockSpec(memory_space=pltpu.VMEM)
        hbm = pl.BlockSpec(memory_space=pl.ANY)
        single = jnp.float32
        dma = pltpu.SemaphoreType.DMA
        square = pltpu.VMEM((width, width), single)
        pair = pltpu.VMEM((2, 1, width), single)
        each = pltpu.VMEM((steps, 1, width), single)
        packed = pl.pallas_call(
            functools.partial(kernel, n_dom, n_sub),
            out_shape=jax.ShapeDtypeStruct((3, width), single),
            in_specs=[vmem, vmem, hbm, hbm, vmem, hbm, hbm, vmem],
            out_specs=vmem,
            scratch_shapes=[
                pltpu.VMEM((2 + blocks, 1, width), single),
                pltpu.VMEM((2, width, width), single),
                pltpu.VMEM((2, width, width), single),
                pltpu.VMEM((2, width, coarse), single),
                pltpu.VMEM((2 * coarse, 2 * coarse), single),
                square, square, square,
                pltpu.VMEM((2 * width, 2 * width), single),
                pltpu.VMEM((2, coarse, width), single),
                pltpu.VMEM((2 * coarse, 2 * coarse), single),
                pair, pair, pair, pair, each, each, each, each,
                pltpu.VMEM((ITERS, 1, LANES), single),
                pltpu.VMEM((ITERS, n_dom, 1, LANES), single),
                pltpu.VMEM((8, width), single),
                pltpu.VMEM((8, width), single),
                pltpu.SemaphoreType.REGULAR,
                dma((4,)), dma, dma, dma((3,)), dma((3,)), dma((3,)), dma((3,)),
                dma((steps,)), dma((steps,)), dma((steps,)), dma((steps,)),
                dma((ITERS,)), dma((ITERS,)), dma, dma,
            ],
            compiler_params=pltpu.CompilerParams(
                collective_id=0, has_side_effects=True, vmem_limit_bytes=GRANT
            ),
        )(
            rhs.reshape(1, width), diagonal.reshape(1, width), self_raw, coupling, pattern,
            prolong, coarse_raw, coarse_diagonal.reshape(1, -1),
        )
        return pl.pallas_call(
            unpack,
            out_shape=(
                jax.ShapeDtypeStruct((width,), single),
                jax.ShapeDtypeStruct((width,), single),
                jax.ShapeDtypeStruct((ITERS,), single),
            ),
            in_specs=[vmem],
            out_specs=(vmem, vmem, vmem),
            compiler_params=pltpu.CompilerParams(vmem_limit_bytes=2**20),
        )(packed)

    line = P(("dom", "sub"))
    table = P(("dom", "sub"), None)
    return jax.shard_map(
        per_device,
        mesh=mesh,
        in_specs=(line, line, table, table, table, table, P("dom", None), P("dom")),
        out_specs=(line, line, P()),
        check_vma=False,
    )
```

```python
import functools

import jax
import jax.numpy as jnp
from jax import lax
from jax.experimental import pallas as pl
from jax.experimental.pallas import tpu as pltpu
from jax.sharding import PartitionSpec as P

ITERS = 3
OMEGA = 0.7
MESH = pl.DeviceIdType.MESH
LANES = 128
GRANT = 56_516_000


def factor(count):
    side = 1
    for trial in range(1, count + 1):
        if trial * trial <= count and count % trial == 0:
            side = trial
    return count // side, side


def fold(matrix, row):
    total = None
    for start in range(0, matrix.shape[1], LANES):
        part = matrix[:, start : start + LANES] * row[:, start : start + LANES]
        total = part if total is None else total + part
    return total


def lanes(block):
    return jnp.sum(block, axis=1, keepdims=True)


def down(matrix, column):
    return jnp.sum(matrix * column, axis=0, keepdims=True)


def product(left, right):
    return jnp.dot(left, right, precision=lax.Precision.HIGHEST, preferred_element_type=jnp.float32)


def eye_of():
    rows = lax.broadcasted_iota(jnp.int32, (LANES, LANES), 0)
    cols = lax.broadcasted_iota(jnp.int32, (LANES, LANES), 1)
    return rows == cols


def embed(row):
    eye = eye_of()
    parts = [
        jnp.where(eye, row[:, start : start + LANES], 0.0) for start in range(0, row.shape[1], LANES)
    ]
    return jnp.concatenate(parts, axis=0)


def upright(row):
    return lanes(embed(row))


def flat(column):
    eye = eye_of()
    parts = [
        jnp.sum(jnp.where(eye, column[start : start + LANES], 0.0), axis=0, keepdims=True)
        for start in range(0, column.shape[0], LANES)
    ]
    return jnp.concatenate(parts, axis=1)


def kernel(
    n_dom, n_sub,
    rhs_ref, diag_ref, self_ref, coup_ref, pat_ref, pro_ref, craw_ref, cdiag_ref,
    out_ref,
    lines, s_raw, c_raw, p_raw, k_raw,
    edge_mat, ft_mat, t_mat, pt_mat, k_mat, q_mat, kt_mat, ke_mat,
    up_out, low_out, up_in, low_in, snd_a, snd_b, in_buf, side_buf, mid_buf, end_buf, rough_buf,
    part_buf, red_buf, pack_out, pack_in,
    known, load_sem, line_send, line_recv, mat_send, mat_recv, edge_send, edge_recv,
    a_send, b_send, in_recv, r_send, r_recv, pack_send, pack_recv,
):
    dom, sub = lax.axis_index("dom"), lax.axis_index("sub")
    width = rhs_ref.shape[1]
    blocks = pat_ref.shape[0]
    brow = width // blocks
    coarse = pro_ref.shape[1]
    has_prev, has_next = dom > 0, dom < n_dom - 1
    n_row, n_col = factor(n_dom)
    barrier = pltpu.get_barrier_semaphore()
    last = ITERS - 1
    lane = lax.broadcasted_iota(jnp.int32, (1, LANES), 1)

    def remote(source, target, send, recv, device):
        return pltpu.make_async_remote_copy(
            source, target, send, recv, device_id=device, device_id_type=MESH
        )

    def line_copy():
        return remote(lines, lines, line_send, line_recv, (dom, 1))

    def mat_copy(index):
        source = (self_ref, coup_ref, pro_ref)[index]
        target = (s_raw, c_raw, p_raw)[index].at[0]
        return remote(source, target, mat_send.at[index], mat_recv.at[index], (dom, 1))

    def pack_copy():
        return remote(pack_out, pack_in, pack_send, pack_recv, (dom, 0))

    def pick(row, place):
        return lanes(jnp.where(lane == place, row[:, :LANES], 0.0))

    def finish(scalars, step, gamma_inv, alpha_inv):
        gamma, delta = pick(scalars, 0), pick(scalars, 1)
        if step == 0:
            return gamma, jnp.zeros_like(gamma), gamma / delta
        beta = gamma * gamma_inv
        return gamma, beta, gamma / (delta - beta * gamma * alpha_inv)

    def put(sol, res, norm_list):
        out_ref[0:1] = sol
        out_ref[1:2] = res
        place_of = lax.broadcasted_iota(jnp.int32, (1, width), 1)
        norms = jnp.zeros((1, width), jnp.float32)
        for step in range(ITERS):
            norms = jnp.where(place_of == step, norm_list[step], norms)
        out_ref[2:3] = norms

    @pl.when(sub == 0)
    def _():
        lines[0] = rhs_ref[...]
        lines[1] = diag_ref[...]
        place = lax.broadcasted_iota(jnp.int32, (1, width), 1)
        for i in range(blocks):
            mask = jnp.zeros((1, width), jnp.float32)
            for j in range(blocks):
                mask = jnp.where(place // brow == j, pat_ref[i : i + 1, j : j + 1].astype(jnp.float32), mask)
            lines[2 + i] = mask
        pl.semaphore_wait(barrier, 1)
        line_copy().start()
        for index in range(3):
            mat_copy(index).start()
        line_copy().wait_send()
        for index in range(3):
            mat_copy(index).wait_send()
        pack_copy().wait_recv()
        sol, resid, uvec, wvec, pvec, svec = [pack_in[index : index + 1] for index in range(6)]
        misc = pack_in[6:7]
        gamma_inv, alpha_inv = 1.0 / pick(misc, 0), 1.0 / pick(misc, 1)
        early = [pick(misc, 2 + step) for step in range(last)]
        every = red_buf.at[last]
        pltpu.make_async_copy(every, every, r_recv.at[last]).wait()
        total = jnp.sum(red_buf[last], axis=0)
        gamma, beta, alpha = finish(total, last, gamma_inv, alpha_inv)
        put(
            sol + alpha * (uvec + beta * pvec),
            resid - alpha * (wvec + beta * svec),
            early + [pick(total, 2)],
        )

    @pl.when(sub == 1)
    def _():
        row_at, col_at = dom // n_col, dom % n_col
        pl.semaphore_signal(barrier, inc=1, device_id=(dom, 0), device_id_type=MESH)

        @pl.when(has_prev)
        def _():
            pl.semaphore_signal(barrier, inc=1, device_id=(dom - 1, 1), device_id_type=MESH)

        @pl.when(has_next)
        def _():
            pl.semaphore_signal(barrier, inc=1, device_id=(dom + 1, 1), device_id_type=MESH)

        def in_row(step):
            return (row_at * n_col + (col_at + step) % n_col, 1)

        def in_col(step):
            return (((row_at + step) % n_row) * n_col + col_at, 1)

        if n_col > 1:
            @pl.loop(1, n_col)
            def _(step):
                pl.semaphore_signal(barrier, inc=1, device_id=in_row(step), device_id_type=MESH)

        @pl.loop(1, n_row)
        def _(step):
            pl.semaphore_signal(barrier, inc=1, device_id=in_col(step), device_id_type=MESH)

        loads = [
            pltpu.make_async_copy(source, target, load_sem.at[index])
            for index, (source, target) in enumerate([
                (coup_ref, c_raw.at[1]), (self_ref, s_raw.at[1]), (pro_ref, p_raw.at[1]), (craw_ref, k_raw),
            ])
        ]
        for load in loads:
            load.start()

        @pl.when(dom == 0)
        def _():
            low_in[...] = jnp.zeros_like(low_in)
            edge_mat[0] = jnp.zeros_like(ft_mat)
            for k in range(1, 3 * ITERS):
                in_buf[k, 0] = jnp.zeros((1, width), jnp.float32)

        @pl.when(dom == n_dom - 1)
        def _():
            up_in[...] = jnp.zeros_like(up_in)
            for k in range(1, 3 * ITERS):
                in_buf[k, 1] = jnp.zeros((1, width), jnp.float32)

        def first_up():
            return remote(up_out, up_in, edge_send.at[0], edge_recv.at[0], (dom - 1, 1))

        def first_low():
            return remote(low_out, low_in, edge_send.at[1], edge_recv.at[1], (dom + 1, 1))

        def edge_matrix():
            return remote(ft_mat, edge_mat.at[0], edge_send.at[2], edge_recv.at[2], (dom + 1, 1))

        def to_prev(k):
            return remote(snd_a.at[k], in_buf.at[k, 1], a_send.at[k], in_recv.at[k, 1], (dom - 1, 1))

        def to_next(k):
            return remote(snd_b.at[k], in_buf.at[k, 0], b_send.at[k], in_recv.at[k, 0], (dom + 1, 1))

        def send(k, vec):
            snd_a[k] = vec[:, :width]
            snd_b[k] = vec[:, width:]

            @pl.when(has_prev)
            def _():
                to_prev(k).start()

            @pl.when(has_next)
            def _():
                to_next(k).start()

        near = 1 - dom % 2
        far = dom % 2
        has_near = jnp.where(near == 1, has_next, has_prev)
        has_far = jnp.where(near == 1, has_prev, has_next)
        order = ((near, has_near), (far, has_far))

        def receive(k, side, exists):
            @pl.when(exists)
            def _():
                landed = in_buf.at[k, side]
                pltpu.make_async_copy(landed, landed, in_recv.at[k, side]).wait()

            return in_buf[k, side]

        loads[0].wait()
        for i in range(blocks):
            for j in range(blocks):
                at = (slice(i * brow, (i + 1) * brow), slice(j * brow, (j + 1) * brow))
                edge_mat[1, at[0], at[1]] = c_raw[1, at[0], at[1]] * pat_ref[i : i + 1, j : j + 1].astype(jnp.float32)
        ft_mat[...] = edge_mat[1].T
        rhs_b, diag_b = rhs_ref[...], diag_ref[...]
        scale_b = OMEGA * (1.0 / diag_b)
        first_b = scale_b * rhs_b
        low_out[0] = down(edge_mat[1], upright(first_b))
        low_out[1] = scale_b

        pl.semaphore_wait(
            barrier,
            (n_row - 1) + (n_col - 1) + has_prev.astype(jnp.int32) + has_next.astype(jnp.int32),
        )

        @pl.loop(1, n_row)
        def _(step):
            pl.semaphore_signal(known, inc=1, device_id=in_col(step), device_id_type=MESH)

        @pl.when(has_next)
        def _():
            first_low().start()

        line_copy().wait_recv()
        rhs_a, diag_a = lines[0], lines[1]
        scale_a = OMEGA * (1.0 / diag_a)
        first_a = scale_a * rhs_a
        up_out[0] = first_a
        up_out[1] = scale_a

        @pl.when(has_prev)
        def _():
            first_up().start()

        @pl.when(has_next)
        def _():
            edge_matrix().start()

        rows = lax.broadcasted_iota(jnp.int32, (width, width), 0)
        cols = lax.broadcasted_iota(jnp.int32, (width, width), 1)
        same = rows == cols

        def put_self(index, diag):
            raw = s_raw[index]
            at = slice(index * width, (index + 1) * width)
            t_mat[index, :, at] = jnp.where(same, diag - diag * (1.0 / OMEGA), 0.5 * (raw + raw.T))

        for load in loads[1:]:
            load.wait()
        put_self(1, diag_b)
        pt_mat[1] = p_raw[1].T
        kinv = 1.0 / cdiag_ref[...]
        craw = k_raw[...]
        k_mat[...] = jnp.where(same, -kinv, (0.5 * (craw + craw.T)) * kinv * upright(kinv))

        rhs = jnp.concatenate([rhs_a, rhs_b], axis=1)
        scale = jnp.concatenate([scale_a, scale_b], axis=1)
        heavy = jnp.concatenate([diag_a, diag_b], axis=1) * (1.0 / OMEGA)
        minus = -upright(scale)

        mat_copy(0).wait_recv()
        put_self(0, diag_a)
        mat_copy(1).wait_recv()
        for i in range(blocks):
            at = slice(i * brow, (i + 1) * brow)
            block = c_raw[0, at, :] * lines[2 + i]
            t_mat[0, at, width:] = block
            t_mat[1, :, at] = block.T
        mat_copy(2).wait_recv()
        pt_mat[0] = p_raw[0].T

        def start_sums(step, resid, uvec, wvec):
            gamma, delta, rnorm = lanes(resid * uvec), lanes(wvec * uvec), lanes(resid * resid)
            line = jnp.where(lane == 0, gamma, jnp.where(lane == 1, delta, rnorm))
            part_buf[step] = line
            red_buf[step, pl.ds(dom, 1)] = line[None]
            if step == 0:
                pl.semaphore_wait(known, n_row - 1)

            @pl.loop(0, n_dom - 1)
            def _(index):
                target = index + (index >= dom).astype(jnp.int32)
                for other in range(n_sub) if step == last else (1,):
                    remote(
                        part_buf.at[step], red_buf.at[step, dom], r_send.at[step], r_recv.at[step],
                        (target, other),
                    ).start()

            if step == last:
                remote(
                    part_buf.at[step], red_buf.at[step, dom], r_send.at[step], r_recv.at[step], (dom, 0)
                ).start()

        def end_sums(step):
            others = red_buf.at[step, pl.ds(0, n_dom - 1)]
            pltpu.make_async_copy(others, others, r_recv.at[step]).wait()
            return jnp.sum(red_buf[step], axis=0)

        def join(buffer):
            return jnp.concatenate([buffer[0], buffer[1]], axis=1)

        def edge_product(side):
            at = slice(side * coarse, (side + 1) * coarse)
            ke_mat[side] = product(k_mat[:, at], product(pt_mat[side], edge_mat[side]))

        def coarse_first(first):
            base_a, base_b = fold(t_mat[0], first), fold(t_mat[1], first)

            def from_prev():
                @pl.when(has_prev)
                def _():
                    first_low().wait_recv()

                rough_buf[0] = down(p_raw[0], lanes(base_a + embed(low_in[0])))

            def from_next():
                @pl.when(has_next)
                def _():
                    first_up().wait_recv()

                rough_buf[1] = down(p_raw[1], lanes(base_b + fold(edge_mat[1], up_in[0])))

            @pl.when(near == 0)
            def _():
                from_prev()
                from_next()

            @pl.when(near == 1)
            def _():
                from_next()
                from_prev()

            return lanes(fold(k_mat[...], join(rough_buf)))

        def coarse_later(k, first):
            base = fold(kt_mat[...], first)
            for side, exists in order:
                base = base + fold(ke_mat[side], receive(k, side, exists))
            return lanes(base)

        def short(vec, second):
            return [
                fold(t_mat[side], second) - embed(vec[:, side * width : (side + 1) * width]) for side in range(2)
            ]

        def across(blocks):
            return jnp.concatenate([flat(lanes(block)) for block in blocks], axis=1)

        def round_of(t, vec, begin, middle):
            first = scale * vec
            if t:
                send(3 * t, first)
            begin()
            if t == 1:
                edge_product(0)
            if t:
                turned = across(short(vec, first))
                etwo = coarse_later(3 * t, first)
            else:
                etwo = coarse_first(first)
            second = first + jnp.concatenate(
                [down(pt_mat[0], etwo[:coarse]), down(pt_mat[1], etwo[coarse:])], axis=1
            )
            send(3 * t + 1, second)
            if t:
                send(3 * t + 2, -scale * (turned + down(q_mat[...], etwo)))
            base = short(vec, second)
            if t == 0:
                send(3 * t + 2, -scale * across(base))
            upper = upright(second)
            side_buf[1] = jnp.where(has_next, up_in[1], 0.0) * down(edge_mat[1], upper[width:])
            if t == 0:
                for side in range(2):
                    q_mat[side * coarse : (side + 1) * coarse] = product(pt_mat[side], t_mat[side])
                kt_mat[...] = product(k_mat[...], q_mat[...])
                edge_product(1)

                @pl.when(has_prev)
                def _():
                    edge_matrix().wait_recv()

            side_buf[0] = jnp.where(has_prev, low_in[1], 0.0) * down(edge_mat[0], upper[:width])
            extra = middle()
            own = None
            for side, exists in order:
                ahead = receive(3 * t + 1, side, exists)
                if t:
                    other = receive(3 * t + 2, side, exists) - side_buf[side]
                total = jnp.where(side == 0, base[0], base[1]) + fold(edge_mat[side], ahead)
                column = jnp.where(side == 0, minus[:width], minus[width:]) * lanes(total)
                part = down(t_mat[side], column)
                own = part if own is None else own + part
                turned = flat(column)
                if not t:
                    other = receive(3 * t + 2, side, exists) - side_buf[side]
                crossed = flat(lanes(fold(edge_mat[side], other)))
                mid_buf[side] = turned
                end_buf[side] = crossed
            mvec = join(mid_buf)
            return mvec, own + heavy * mvec + join(end_buf), extra

        resid = rhs
        uvec, wvec, _ = round_of(0, resid, lambda: None, lambda: None)
        zeros = jnp.zeros_like(resid)
        pvec, svec, qvec, zvec, solution = (zeros,) * 5
        norm_list = []
        gamma_inv = alpha_inv = None
        for step in range(last):
            def begin():
                start_sums(step, resid, uvec, wvec)

            def middle():
                sums = end_sums(step)
                return sums, finish(sums, step, gamma_inv, alpha_inv)

            mvec, nvec, (total, (gamma, beta, alpha)) = round_of(step + 1, wvec, begin, middle)
            gamma_inv, alpha_inv = 1.0 / gamma, 1.0 / alpha
            norm_list.append(pick(total, 2))
            svec = wvec + beta * svec
            pvec = uvec + beta * pvec
            solution = solution + alpha * pvec
            resid = resid - alpha * svec
            zvec = nvec + beta * zvec
            qvec = mvec + beta * qvec
            uvec = uvec - alpha * qvec
            wvec = wvec - alpha * zvec
        start_sums(last, resid, uvec, wvec)
        for index, vec in enumerate([solution, resid, uvec, wvec, pvec, svec]):
            pack_out[index : index + 1] = vec[:, :width]
        misc = jnp.where(lane == 0, gamma, alpha)
        for step in range(last):
            misc = jnp.where(lane == 2 + step, norm_list[step], misc)
        pack_out[6:7, :LANES] = misc
        pack_copy().start()
        total = end_sums(last)
        gamma, beta, alpha = finish(total, last, gamma_inv, alpha_inv)
        put(
            (solution + alpha * (uvec + beta * pvec))[:, width:],
            (resid - alpha * (wvec + beta * svec))[:, width:],
            norm_list + [pick(total, 2)],
        )

        pack_copy().wait_send()

        @pl.when(has_prev)
        def _():
            first_up().wait_send()
            for k in range(1, 3 * ITERS):
                to_prev(k).wait_send()

        @pl.when(has_next)
        def _():
            first_low().wait_send()
            edge_matrix().wait_send()
            for k in range(1, 3 * ITERS):
                to_next(k).wait_send()

        for step in range(ITERS):
            sent = red_buf.at[step, pl.ds(0, n_dom - 1)]
            pltpu.make_async_copy(sent, sent, r_send.at[step]).wait()
            if step == last:
                every = red_buf.at[step]
                pltpu.make_async_copy(every, every, r_send.at[step]).wait()


def unpack(packed_ref, sol_ref, res_ref, norm_ref):
    sol_ref[...] = packed_ref[0]
    res_ref[...] = packed_ref[1]
    norm_ref[...] = packed_ref[2, : norm_ref.shape[0]]


def solution(mesh):
    n_dom, n_sub = mesh.shape["dom"], mesh.shape["sub"]

    def per_device(rhs, diagonal, self_raw, coupling, pattern, prolong, coarse_raw, coarse_diagonal):
        width = rhs.shape[0]
        coarse = prolong.shape[1]
        blocks = pattern.shape[0]
        steps = 3 * ITERS
        vmem = pl.BlockSpec(memory_space=pltpu.VMEM)
        hbm = pl.BlockSpec(memory_space=pl.ANY)
        single = jnp.float32
        dma = pltpu.SemaphoreType.DMA
        square = pltpu.VMEM((width, width), single)
        pair = pltpu.VMEM((2, 1, width), single)
        each = pltpu.VMEM((steps, 1, width), single)
        packed = pl.pallas_call(
            functools.partial(kernel, n_dom, n_sub),
            out_shape=jax.ShapeDtypeStruct((3, width), single),
            in_specs=[vmem, vmem, hbm, hbm, vmem, hbm, hbm, vmem],
            out_specs=vmem,
            scratch_shapes=[
                pltpu.VMEM((2 + blocks, 1, width), single),
                pltpu.VMEM((2, width, width), single),
                pltpu.VMEM((2, width, width), single),
                pltpu.VMEM((2, width, coarse), single),
                pltpu.VMEM((2 * coarse, 2 * coarse), single),
                pltpu.VMEM((2, width, width), single),
                square,
                pltpu.VMEM((2, width, 2 * width), single),
                pltpu.VMEM((2, coarse, width), single),
                pltpu.VMEM((2 * coarse, 2 * coarse), single),
                pltpu.VMEM((2 * coarse, 2 * width), single),
                pltpu.VMEM((2 * coarse, 2 * width), single),
                pltpu.VMEM((2, 2 * coarse, width), single),
                pair, pair, pair, pair, each, each,
                pltpu.VMEM((steps, 2, 1, width), single),
                pair, pair, pair,
                pltpu.VMEM((2, 1, coarse), single),
                pltpu.VMEM((ITERS, 1, LANES), single),
                pltpu.VMEM((ITERS, n_dom, 1, LANES), single),
                pltpu.VMEM((8, width), single),
                pltpu.VMEM((8, width), single),
                pltpu.SemaphoreType.REGULAR,
                dma((4,)), dma, dma, dma((3,)), dma((3,)), dma((3,)), dma((3,)),
                dma((steps,)), dma((steps,)), dma((steps, 2)),
                dma((ITERS,)), dma((ITERS,)), dma, dma,
            ],
            compiler_params=pltpu.CompilerParams(
                collective_id=0, has_side_effects=True, vmem_limit_bytes=GRANT
            ),
        )(
            rhs.reshape(1, width), diagonal.reshape(1, width), self_raw, coupling, pattern,
            prolong, coarse_raw, coarse_diagonal.reshape(1, -1),
        )
        return pl.pallas_call(
            unpack,
            out_shape=(
                jax.ShapeDtypeStruct((width,), single),
                jax.ShapeDtypeStruct((width,), single),
                jax.ShapeDtypeStruct((ITERS,), single),
            ),
            in_specs=[vmem],
            out_specs=(vmem, vmem, vmem),
            compiler_params=pltpu.CompilerParams(vmem_limit_bytes=2**20),
        )(packed)

    line = P(("dom", "sub"))
    table = P(("dom", "sub"), None)
    return jax.shard_map(
        per_device,
        mesh=mesh,
        in_specs=(line, line, table, table, table, table, P("dom", None), P("dom")),
        out_specs=(line, line, P()),
        check_vma=False,
    )
```

```python
import functools

import jax
import jax.numpy as jnp
from jax import lax
from jax.experimental import pallas as pl
from jax.experimental.pallas import tpu as pltpu
from jax.sharding import PartitionSpec as P

ITERS = 3
OMEGA = 0.7
MESH = pl.DeviceIdType.MESH
LANES = 128
GRANT = 56_516_000


def factor(count):
    side = 1
    for trial in range(1, count + 1):
        if trial * trial <= count and count % trial == 0:
            side = trial
    return count // side, side


def fold(matrix, row):
    total = None
    for start in range(0, matrix.shape[1], LANES):
        part = matrix[:, start : start + LANES] * row[:, start : start + LANES]
        total = part if total is None else total + part
    return total


def lanes(block):
    return jnp.sum(block, axis=1, keepdims=True)


def down(matrix, column):
    return jnp.sum(matrix * column, axis=0, keepdims=True)


def product(left, right):
    return jnp.dot(left, right, precision=lax.Precision.HIGHEST, preferred_element_type=jnp.float32)


def eye_of():
    rows = lax.broadcasted_iota(jnp.int32, (LANES, LANES), 0)
    cols = lax.broadcasted_iota(jnp.int32, (LANES, LANES), 1)
    return rows == cols


def embed(row):
    eye = eye_of()
    parts = [
        jnp.where(eye, row[:, start : start + LANES], 0.0) for start in range(0, row.shape[1], LANES)
    ]
    return jnp.concatenate(parts, axis=0)


def upright(row):
    return lanes(embed(row))


def flat(column):
    eye = eye_of()
    parts = [
        jnp.sum(jnp.where(eye, column[start : start + LANES], 0.0), axis=0, keepdims=True)
        for start in range(0, column.shape[0], LANES)
    ]
    return jnp.concatenate(parts, axis=1)


def kernel(
    n_dom, n_sub,
    rhs_ref, diag_ref, self_ref, coup_ref, pat_ref, pro_ref, craw_ref, cdiag_ref,
    out_ref,
    lines, s_raw, c_raw, p_raw, k_raw,
    edge_mat, ft_mat, t_mat, pt_mat, k_mat, q_mat, kt_mat, ke_mat,
    up_out, low_out, up_in, low_in, out_buf, in_buf, side_buf, mid_buf, end_buf, rough_buf,
    part_buf, red_buf, pack_out, pack_in, halo_mat,
    known, go, load_sem, line_send, line_recv, mat_send, mat_recv, edge_send, edge_recv,
    out_send, in_recv, r_send, r_recv, pack_send, pack_recv, halo_send, halo_recv, stage_send, stage_recv,
):
    dom, sub = lax.axis_index("dom"), lax.axis_index("sub")
    width = rhs_ref.shape[1]
    blocks = pat_ref.shape[0]
    brow = width // blocks
    coarse = pro_ref.shape[1]
    has_prev, has_next = dom > 0, dom < n_dom - 1
    n_row, n_col = factor(n_dom)
    barrier = pltpu.get_barrier_semaphore()
    last = ITERS - 1
    far = dom % 2
    near = 1 - far
    beyond = dom + 2 * far - 1
    relays = n_col % 2 == 0
    wide = jnp.logical_or(
        jnp.logical_and(has_prev, dom % n_col == 0), jnp.logical_and(has_next, dom % n_col == n_col - 1)
    )
    lane = lax.broadcasted_iota(jnp.int32, (1, LANES), 1)

    def remote(source, target, send, recv, device):
        return pltpu.make_async_remote_copy(
            source, target, send, recv, device_id=device, device_id_type=MESH
        )

    def line_copy():
        return remote(lines, lines, line_send, line_recv, (dom, 1))

    def mat_copy(index):
        source = (self_ref, coup_ref, pro_ref)[index]
        target = (s_raw, c_raw, p_raw)[index].at[0]
        return remote(source, target, mat_send.at[index], mat_recv.at[index], (dom, 1))

    def pack_copy():
        return remote(pack_out, pack_in, pack_send, pack_recv, (dom, 0))

    def pick(row, place):
        return lanes(jnp.where(lane == place, row[:, :LANES], 0.0))

    def stage_copy():
        return remote(s_raw.at[1], halo_mat, stage_send, stage_recv, (dom, 0))

    def halo_copy(source):
        return remote(source, halo_mat, halo_send, halo_recv, (beyond, 1))

    def finish(scalars, step, gamma_inv, alpha_inv):
        gamma, delta = pick(scalars, 0), pick(scalars, 1)
        if step == 0:
            return gamma, jnp.zeros_like(gamma), gamma / delta
        beta = gamma * gamma_inv
        return gamma, beta, gamma / (delta - beta * gamma * alpha_inv)

    def put(sol, res, norm_list):
        out_ref[0:1] = sol
        out_ref[1:2] = res
        place_of = lax.broadcasted_iota(jnp.int32, (1, width), 1)
        norms = jnp.zeros((1, width), jnp.float32)
        for step in range(ITERS):
            norms = jnp.where(place_of == step, norm_list[step], norms)
        out_ref[2:3] = norms

    @pl.when(sub == 0)
    def _():
        lines[0] = rhs_ref[...]
        lines[1] = diag_ref[...]
        place = lax.broadcasted_iota(jnp.int32, (1, width), 1)
        for i in range(blocks):
            mask = jnp.zeros((1, width), jnp.float32)
            for j in range(blocks):
                mask = jnp.where(place // brow == j, pat_ref[i : i + 1, j : j + 1].astype(jnp.float32), mask)
            lines[2 + i] = mask
        pl.semaphore_wait(barrier, 1)
        line_copy().start()
        for index in range(3):
            mat_copy(index).start()
        if relays:
            @pl.when(wide)
            def _():
                pl.semaphore_wait(go, 1)

                @pl.when(far == 0)
                def _():
                    halo_copy(self_ref).start()

                @pl.when(far == 1)
                def _():
                    stage_copy().wait_recv()
                    halo_copy(halo_mat).start()

        line_copy().wait_send()
        for index in range(3):
            mat_copy(index).wait_send()
        if relays:
            @pl.when(wide)
            def _():
                halo_copy(halo_mat).wait_send()

        pack_copy().wait_recv()
        sol, resid, uvec, wvec, pvec, svec = [pack_in[index : index + 1] for index in range(6)]
        misc = pack_in[6:7]
        gamma_inv, alpha_inv = 1.0 / pick(misc, 0), 1.0 / pick(misc, 1)
        early = [pick(misc, 2 + step) for step in range(last)]
        every = red_buf.at[last]
        pltpu.make_async_copy(every, every, r_recv.at[last]).wait()
        total = jnp.sum(red_buf[last], axis=0)
        gamma, beta, alpha = finish(total, last, gamma_inv, alpha_inv)
        put(
            sol + alpha * (uvec + beta * pvec),
            resid - alpha * (wvec + beta * svec),
            early + [pick(total, 2)],
        )

    @pl.when(sub == 1)
    def _():
        row_at, col_at = dom // n_col, dom % n_col
        pl.semaphore_signal(barrier, inc=1, device_id=(dom, 0), device_id_type=MESH)

        @pl.when(has_prev)
        def _():
            pl.semaphore_signal(barrier, inc=1, device_id=(dom - 1, 1), device_id_type=MESH)

        @pl.when(has_next)
        def _():
            pl.semaphore_signal(barrier, inc=1, device_id=(dom + 1, 1), device_id_type=MESH)

        def in_row(step):
            return (row_at * n_col + (col_at + step) % n_col, 1)

        def in_col(step):
            return (((row_at + step) % n_row) * n_col + col_at, 1)

        if n_col > 1:
            @pl.loop(1, n_col)
            def _(step):
                pl.semaphore_signal(barrier, inc=1, device_id=in_row(step), device_id_type=MESH)

        @pl.loop(1, n_row)
        def _(step):
            pl.semaphore_signal(barrier, inc=1, device_id=in_col(step), device_id_type=MESH)

        loads = [
            pltpu.make_async_copy(source, target, load_sem.at[index])
            for index, (source, target) in enumerate([
                (coup_ref, c_raw.at[1]), (self_ref, s_raw.at[1]), (pro_ref, p_raw.at[1]), (craw_ref, k_raw),
            ])
        ]
        for load in loads:
            load.start()

        @pl.when(dom == 0)
        def _():
            low_in[...] = jnp.zeros_like(low_in)
            edge_mat[0] = jnp.zeros_like(ft_mat)
            for k in range(1, 3 * ITERS):
                in_buf[k, 0] = jnp.zeros((1, width), jnp.float32)

        @pl.when(dom == n_dom - 1)
        def _():
            up_in[...] = jnp.zeros_like(up_in)
            for k in range(1, 3 * ITERS):
                in_buf[k, 1] = jnp.zeros((1, width), jnp.float32)

        def first_up():
            return remote(up_out, up_in, edge_send.at[0], edge_recv.at[0], (dom - 1, 1))

        def first_low():
            return remote(low_out, low_in, edge_send.at[1], edge_recv.at[1], (dom + 1, 1))

        def edge_matrix():
            return remote(ft_mat, edge_mat.at[0], edge_send.at[2], edge_recv.at[2], (dom + 1, 1))

        def to_side(k, side, place=None):
            source = out_buf.at[k if place is None else place, side]
            return remote(
                source, in_buf.at[k, 1 - side], out_send.at[k, side], in_recv.at[k, 1 - side], (dom + 2 * side - 1, 1)
            )

        def send(k, vec, wanted=(has_prev, has_next)):
            for side in range(2):
                out_buf[k, side] = vec[:, side * width : (side + 1) * width]

                @pl.when(wanted[side])
                def _():
                    to_side(k, side).start()

        has_near = jnp.where(near == 1, has_next, has_prev)
        has_far = jnp.where(near == 1, has_prev, has_next)
        order = ((near, has_near), (far, has_far))

        def receive(k, side, exists):
            @pl.when(exists)
            def _():
                landed = in_buf.at[k, side]
                pltpu.make_async_copy(landed, landed, in_recv.at[k, side]).wait()

            return in_buf[k, side]

        loads[0].wait()
        for i in range(blocks):
            for j in range(blocks):
                at = (slice(i * brow, (i + 1) * brow), slice(j * brow, (j + 1) * brow))
                edge_mat[1, at[0], at[1]] = c_raw[1, at[0], at[1]] * pat_ref[i : i + 1, j : j + 1].astype(jnp.float32)
        ft_mat[...] = edge_mat[1].T
        rhs_b, diag_b = rhs_ref[...], diag_ref[...]
        scale_b = OMEGA * (1.0 / diag_b)
        first_b = scale_b * rhs_b
        low_out[0] = down(edge_mat[1], upright(first_b))
        low_out[1] = scale_b

        pl.semaphore_wait(
            barrier,
            (n_row - 1) + (n_col - 1) + has_prev.astype(jnp.int32) + has_next.astype(jnp.int32),
        )

        @pl.loop(1, n_row)
        def _(step):
            pl.semaphore_signal(known, inc=1, device_id=in_col(step), device_id_type=MESH)

        @pl.when(has_next)
        def _():
            first_low().start()

        line_copy().wait_recv()
        rhs_a, diag_a = lines[0], lines[1]
        scale_a = OMEGA * (1.0 / diag_a)
        first_a = scale_a * rhs_a
        up_out[0] = first_a
        up_out[1] = scale_a

        @pl.when(has_prev)
        def _():
            first_up().start()

        @pl.when(has_next)
        def _():
            edge_matrix().start()

        rows = lax.broadcasted_iota(jnp.int32, (width, width), 0)
        cols = lax.broadcasted_iota(jnp.int32, (width, width), 1)
        same = rows == cols

        def put_self(index, diag):
            raw = s_raw[index]
            at = slice(index * width, (index + 1) * width)
            t_mat[index, :, at] = jnp.where(same, diag - diag * (1.0 / OMEGA), 0.5 * (raw + raw.T))

        for load in loads[1:]:
            load.wait()
        if relays:
            @pl.when(jnp.logical_and(wide, far == 1))
            def _():
                stage_copy().start()

            @pl.when(jnp.logical_not(wide))
            def _():
                halo_mat[...] = jnp.zeros_like(halo_mat)

        put_self(1, diag_b)
        pt_mat[1] = p_raw[1].T
        kinv = 1.0 / cdiag_ref[...]
        craw = k_raw[...]
        k_mat[...] = jnp.where(same, -kinv, (0.5 * (craw + craw.T)) * kinv * upright(kinv))

        rhs = jnp.concatenate([rhs_a, rhs_b], axis=1)
        scale = jnp.concatenate([scale_a, scale_b], axis=1)
        heavy = jnp.concatenate([diag_a, diag_b], axis=1) * (1.0 / OMEGA)
        minus = -upright(scale)

        mat_copy(0).wait_recv()
        put_self(0, diag_a)
        mat_copy(1).wait_recv()
        for i in range(blocks):
            at = slice(i * brow, (i + 1) * brow)
            block = c_raw[0, at, :] * lines[2 + i]
            t_mat[0, at, width:] = block
            t_mat[1, :, at] = block.T
        mat_copy(2).wait_recv()
        pt_mat[0] = p_raw[0].T

        def start_sums(step, resid, uvec, wvec):
            gamma, delta, rnorm = lanes(resid * uvec), lanes(wvec * uvec), lanes(resid * resid)
            line = jnp.where(lane == 0, gamma, jnp.where(lane == 1, delta, rnorm))
            part_buf[step] = line
            red_buf[step, pl.ds(dom, 1)] = line[None]
            if step == 0:
                pl.semaphore_wait(known, n_row - 1)

            @pl.loop(0, n_dom - 1)
            def _(index):
                target = index + (index >= dom).astype(jnp.int32)
                for other in range(n_sub) if step == last else (1,):
                    remote(
                        part_buf.at[step], red_buf.at[step, dom], r_send.at[step], r_recv.at[step],
                        (target, other),
                    ).start()

            if step == last:
                remote(
                    part_buf.at[step], red_buf.at[step, dom], r_send.at[step], r_recv.at[step], (dom, 0)
                ).start()

        def end_sums(step):
            others = red_buf.at[step, pl.ds(0, n_dom - 1)]
            pltpu.make_async_copy(others, others, r_recv.at[step]).wait()
            return jnp.sum(red_buf[step], axis=0)

        def join(buffer):
            return jnp.concatenate([buffer[0], buffer[1]], axis=1)

        def edge_product(side):
            at = slice(side * coarse, (side + 1) * coarse)
            ke_mat[side] = product(k_mat[:, at], product(pt_mat[side], edge_mat[side]))

        def coarse_first(first):
            base_a, base_b = fold(t_mat[0], first), fold(t_mat[1], first)

            def from_prev():
                @pl.when(has_prev)
                def _():
                    first_low().wait_recv()

                rough_buf[0] = down(p_raw[0], lanes(base_a + embed(low_in[0])))

            def from_next():
                @pl.when(has_next)
                def _():
                    first_up().wait_recv()

                rough_buf[1] = down(p_raw[1], lanes(base_b + fold(edge_mat[1], up_in[0])))

            @pl.when(near == 0)
            def _():
                from_prev()
                from_next()

            @pl.when(near == 1)
            def _():
                from_next()
                from_prev()

            return lanes(fold(k_mat[...], join(rough_buf)))

        def half(vec):
            return jnp.where(far == 0, vec[:, :width], vec[:, width:])

        def coarse_later(k, first, halo):
            base = fold(kt_mat[...], first)
            for side, exists in order:
                row = receive(k, side, exists)
                if halo is not None and side is far:
                    row = jnp.where(wide, halo[0] - halo[1] * row, row)
                base = base + fold(ke_mat[side], row)
            return lanes(base)

        def short(vec, second):
            return [
                fold(t_mat[side], second) - embed(vec[:, side * width : (side + 1) * width]) for side in range(2)
            ]

        def across(blocks):
            return jnp.concatenate([flat(lanes(block)) for block in blocks], axis=1)

        def round_of(t, vec, begin, middle, held=None):
            first = scale * vec
            halo = None
            if held is not None:
                send(3 * t, first, (
                    jnp.logical_and(has_prev, dom % n_col != 0), jnp.logical_and(has_next, dom % n_col != n_col - 1)
                ))
            elif t:
                send(3 * t, first)
            begin()
            if held is not None:
                column, strong, step_size = held
                pull = step_size * far_scale
                halo = in_buf[3, far] - pull * (down(edge_mat[far], column) - strong), pull
            if t == 1:
                edge_product(0)
            if t:
                turned = across(short(vec, first))
                etwo = coarse_later(3 * t, first, halo)
            else:
                etwo = coarse_first(first)
            second = first + jnp.concatenate(
                [down(pt_mat[0], etwo[:coarse]), down(pt_mat[1], etwo[coarse:])], axis=1
            )
            send(3 * t + 1, second)
            if t:
                ghost = -scale * (turned + down(q_mat[...], etwo))
                send(3 * t + 2, ghost)
            base = short(vec, second)
            if t == 0:
                send(3 * t + 2, -scale * across(base))

                @pl.when(has_next)
                def _():
                    edge_matrix().wait_send()

                if relays:
                    @pl.when(wide)
                    def _():
                        pl.semaphore_signal(go, inc=1, device_id=(dom, 0), device_id_type=MESH)

            upper = upright(second)
            side_buf[1] = jnp.where(has_next, up_in[1], 0.0) * down(edge_mat[1], upper[width:])
            if t == 0:
                for side in range(2):
                    q_mat[side * coarse : (side + 1) * coarse] = product(pt_mat[side], t_mat[side])
                kt_mat[...] = product(k_mat[...], q_mat[...])
                edge_product(1)

                @pl.when(has_prev)
                def _():
                    edge_matrix().wait_recv()

            side_buf[0] = jnp.where(has_prev, low_in[1], 0.0) * down(edge_mat[0], upper[:width])
            extra = middle()
            early = relays and t == 1
            if early:
                blank = jnp.zeros((1, width), jnp.float32)
                alone = jnp.concatenate(
                    [jnp.where(far == 0, ghost[:, :width], blank), jnp.where(far == 0, blank, ghost[:, width:])], axis=1
                )
                mine = flat(lanes(fold(t_mat[far], alone))) + half(heavy) * half(ghost)

                @pl.when(wide)
                def _():
                    halo_copy(halo_mat).wait_recv()

                bare = jnp.where(same, 0.0, halo_mat[...])
                lost = side_buf[far]
                strong = 0.5 * (flat(lanes(fold(bare, lost))) + down(bare, upright(lost))) + far_diag * lost
            own = None
            for side, exists in order:
                ahead = receive(3 * t + 1, side, exists)
                if t:
                    other = receive(3 * t + 2, side, exists) - side_buf[side]
                total = jnp.where(side == 0, base[0], base[1]) + fold(edge_mat[side], ahead)
                column = jnp.where(side == 0, minus[:width], minus[width:]) * lanes(total)
                part = down(t_mat[side], column)
                if early and side is near:
                    @pl.when(wide)
                    def _():
                        out_buf[3 * ITERS, far] = half(part) + mine
                        to_side(3 * t + 3, far, 3 * ITERS).start()

                own = part if own is None else own + part
                turned = flat(column)
                if not t:
                    other = receive(3 * t + 2, side, exists) - side_buf[side]
                crossed = flat(lanes(fold(edge_mat[side], other)))
                mid_buf[side] = turned
                end_buf[side] = crossed
            mvec = join(mid_buf)
            return mvec, own + heavy * mvec + join(end_buf), extra, (column, strong) if early else None

        resid = rhs
        uvec, wvec, _, _ = round_of(0, resid, lambda: None, lambda: None)
        far_scale = jnp.where(far == 0, low_in[1], up_in[1])
        far_diag = OMEGA / far_scale
        held = None
        zeros = jnp.zeros_like(resid)
        pvec, svec, qvec, zvec, solution = (zeros,) * 5
        norm_list = []
        gamma_inv = alpha_inv = None
        for step in range(last):
            def begin():
                start_sums(step, resid, uvec, wvec)

            def middle():
                sums = end_sums(step)
                return sums, finish(sums, step, gamma_inv, alpha_inv)

            mvec, nvec, (total, (gamma, beta, alpha)), kept = round_of(step + 1, wvec, begin, middle, held)
            held = None if kept is None else kept + (alpha,)
            gamma_inv, alpha_inv = 1.0 / gamma, 1.0 / alpha
            norm_list.append(pick(total, 2))
            svec = wvec + beta * svec
            pvec = uvec + beta * pvec
            solution = solution + alpha * pvec
            resid = resid - alpha * svec
            zvec = nvec + beta * zvec
            qvec = mvec + beta * qvec
            uvec = uvec - alpha * qvec
            wvec = wvec - alpha * zvec
        start_sums(last, resid, uvec, wvec)
        for index, vec in enumerate([solution, resid, uvec, wvec, pvec, svec]):
            pack_out[index : index + 1] = vec[:, :width]
        misc = jnp.where(lane == 0, gamma, alpha)
        for step in range(last):
            misc = jnp.where(lane == 2 + step, norm_list[step], misc)
        pack_out[6:7, :LANES] = misc
        pack_copy().start()
        total = end_sums(last)
        gamma, beta, alpha = finish(total, last, gamma_inv, alpha_inv)
        put(
            (solution + alpha * (uvec + beta * pvec))[:, width:],
            (resid - alpha * (wvec + beta * svec))[:, width:],
            norm_list + [pick(total, 2)],
        )

        pack_copy().wait_send()
        if relays:
            @pl.when(jnp.logical_and(wide, far == 1))
            def _():
                stage_copy().wait_send()

        @pl.when(has_prev)
        def _():
            first_up().wait_send()
            for k in range(1, 3 * ITERS):
                to_side(k, 0).wait_send()

        @pl.when(has_next)
        def _():
            first_low().wait_send()
            for k in range(1, 3 * ITERS):
                to_side(k, 1).wait_send()

        for step in range(ITERS):
            sent = red_buf.at[step, pl.ds(0, n_dom - 1)]
            pltpu.make_async_copy(sent, sent, r_send.at[step]).wait()
            if step == last:
                every = red_buf.at[step]
                pltpu.make_async_copy(every, every, r_send.at[step]).wait()


def unpack(packed_ref, sol_ref, res_ref, norm_ref):
    sol_ref[...] = packed_ref[0]
    res_ref[...] = packed_ref[1]
    norm_ref[...] = packed_ref[2, : norm_ref.shape[0]]


def solution(mesh):
    n_dom, n_sub = mesh.shape["dom"], mesh.shape["sub"]

    def per_device(rhs, diagonal, self_raw, coupling, pattern, prolong, coarse_raw, coarse_diagonal):
        width = rhs.shape[0]
        coarse = prolong.shape[1]
        blocks = pattern.shape[0]
        steps = 3 * ITERS
        vmem = pl.BlockSpec(memory_space=pltpu.VMEM)
        hbm = pl.BlockSpec(memory_space=pl.ANY)
        single = jnp.float32
        dma = pltpu.SemaphoreType.DMA
        square = pltpu.VMEM((width, width), single)
        pair = pltpu.VMEM((2, 1, width), single)
        packed = pl.pallas_call(
            functools.partial(kernel, n_dom, n_sub),
            out_shape=jax.ShapeDtypeStruct((3, width), single),
            in_specs=[vmem, vmem, hbm, hbm, vmem, hbm, hbm, vmem],
            out_specs=vmem,
            scratch_shapes=[
                pltpu.VMEM((2 + blocks, 1, width), single),
                pltpu.VMEM((2, width, width), single),
                pltpu.VMEM((2, width, width), single),
                pltpu.VMEM((2, width, coarse), single),
                pltpu.VMEM((2 * coarse, 2 * coarse), single),
                pltpu.VMEM((2, width, width), single),
                square,
                pltpu.VMEM((2, width, 2 * width), single),
                pltpu.VMEM((2, coarse, width), single),
                pltpu.VMEM((2 * coarse, 2 * coarse), single),
                pltpu.VMEM((2 * coarse, 2 * width), single),
                pltpu.VMEM((2 * coarse, 2 * width), single),
                pltpu.VMEM((2, 2 * coarse, width), single),
                pair, pair, pair, pair,
                pltpu.VMEM((steps + 1, 2, 1, width), single),
                pltpu.VMEM((steps, 2, 1, width), single),
                pair, pair, pair,
                pltpu.VMEM((2, 1, coarse), single),
                pltpu.VMEM((ITERS, 1, LANES), single),
                pltpu.VMEM((ITERS, n_dom, 1, LANES), single),
                pltpu.VMEM((8, width), single),
                pltpu.VMEM((8, width), single),
                square,
                pltpu.SemaphoreType.REGULAR, pltpu.SemaphoreType.REGULAR,
                dma((4,)), dma, dma, dma((3,)), dma((3,)), dma((3,)), dma((3,)),
                dma((steps, 2)), dma((steps, 2)),
                dma((ITERS,)), dma((ITERS,)), dma, dma, dma, dma, dma, dma,
            ],
            compiler_params=pltpu.CompilerParams(
                collective_id=0, has_side_effects=True, vmem_limit_bytes=GRANT
            ),
        )(
            rhs.reshape(1, width), diagonal.reshape(1, width), self_raw, coupling, pattern,
            prolong, coarse_raw, coarse_diagonal.reshape(1, -1),
        )
        return pl.pallas_call(
            unpack,
            out_shape=(
                jax.ShapeDtypeStruct((width,), single),
                jax.ShapeDtypeStruct((width,), single),
                jax.ShapeDtypeStruct((ITERS,), single),
            ),
            in_specs=[vmem],
            out_specs=(vmem, vmem, vmem),
            compiler_params=pltpu.CompilerParams(vmem_limit_bytes=2**20),
        )(packed)

    line = P(("dom", "sub"))
    table = P(("dom", "sub"), None)
    return jax.shard_map(
        per_device,
        mesh=mesh,
        in_specs=(line, line, table, table, table, table, P("dom", None), P("dom")),
        out_specs=(line, line, P()),
        check_vma=False,
    )
```

```python
import functools

import jax
import jax.numpy as jnp
from jax import lax
from jax.experimental import pallas as pl
from jax.experimental.pallas import tpu as pltpu
from jax.sharding import PartitionSpec as P

ITERS = 3
OMEGA = 0.7
MESH = pl.DeviceIdType.MESH
LANES = 128
GRANT = 56_516_000


def factor(count):
    side = 1
    for trial in range(1, count + 1):
        if trial * trial <= count and count % trial == 0:
            side = trial
    return count // side, side


def fold(matrix, row):
    total = None
    for start in range(0, matrix.shape[1], LANES):
        part = matrix[:, start : start + LANES] * row[:, start : start + LANES]
        total = part if total is None else total + part
    return total


def lanes(block):
    return jnp.sum(block, axis=1, keepdims=True)


def down(matrix, column):
    return jnp.sum(matrix * column, axis=0, keepdims=True)


def times(left, right):
    if isinstance(left, float) and left in (0.0, 1.0):
        return right if left else 0.0
    if isinstance(right, float) and right in (0.0, 1.0):
        return left if right else 0.0
    return left * right


def plus(left, right):
    if isinstance(left, float) and left == 0.0:
        return right
    if isinstance(right, float) and right == 0.0:
        return left
    return left + right


def blend(scale, left, right):
    return [plus(one, times(scale, other)) for one, other in zip(right, left)]


def combine(weights, terms):
    total = 0.0
    for weight, term in zip(weights, terms):
        total = plus(total, times(weight, term))
    return total


def shift(row):
    return [plus(row[k], times(-1.0, row[k - 1])) if k else row[0] for k in range(len(row))]


def product(left, right):
    return jnp.dot(left, right, precision=lax.Precision.HIGHEST, preferred_element_type=jnp.float32)


def eye_of():
    rows = lax.broadcasted_iota(jnp.int32, (LANES, LANES), 0)
    cols = lax.broadcasted_iota(jnp.int32, (LANES, LANES), 1)
    return rows == cols


def embed(row):
    eye = eye_of()
    parts = [
        jnp.where(eye, row[:, start : start + LANES], 0.0) for start in range(0, row.shape[1], LANES)
    ]
    return jnp.concatenate(parts, axis=0)


def upright(row):
    return lanes(embed(row))


def flat(column):
    eye = eye_of()
    parts = [
        jnp.sum(jnp.where(eye, column[start : start + LANES], 0.0), axis=0, keepdims=True)
        for start in range(0, column.shape[0], LANES)
    ]
    return jnp.concatenate(parts, axis=1)


def kernel(
    n_dom, n_sub,
    rhs_ref, diag_ref, self_ref, coup_ref, pat_ref, pro_ref, craw_ref, cdiag_ref,
    out_ref,
    lines, s_raw, c_raw, p_raw, k_raw,
    edge_mat, ft_mat, t_mat, pt_mat, k_mat, q_mat, kt_mat, ke_mat,
    up_out, low_out, up_in, low_in, out_buf, in_buf, rim_buf, side_buf, mid_buf, end_buf, rough_buf,
    part_buf, red_buf, pack_out, pack_in, halo_mat,
    met, known, go, load_sem, line_send, line_recv, mat_send, mat_recv, edge_send, edge_recv,
    out_send, in_recv, r_send, r_recv, pack_send, pack_recv, halo_send, halo_recv, stage_send, stage_recv,
):
    dom, sub = lax.axis_index("dom"), lax.axis_index("sub")
    width = rhs_ref.shape[1]
    blocks = pat_ref.shape[0]
    brow = width // blocks
    coarse = pro_ref.shape[1]
    has_prev, has_next = dom > 0, dom < n_dom - 1
    n_row, n_col = factor(n_dom)
    barrier = pltpu.get_barrier_semaphore()
    first_sums, last_sums = range(2)
    last = ITERS - 1
    far = dom % 2
    near = 1 - far
    beyond = dom + 2 * far - 1
    relays = n_col % 2 == 0
    wide = jnp.logical_or(
        jnp.logical_and(has_prev, dom % n_col == 0), jnp.logical_and(has_next, dom % n_col == n_col - 1)
    )
    lane = lax.broadcasted_iota(jnp.int32, (1, LANES), 1)

    def remote(source, target, send, recv, device):
        return pltpu.make_async_remote_copy(
            source, target, send, recv, device_id=device, device_id_type=MESH
        )

    def line_copy():
        return remote(lines, lines, line_send, line_recv, (dom, 1))

    def mat_copy(index):
        source = (self_ref, coup_ref, pro_ref)[index]
        target = (s_raw, c_raw, p_raw)[index].at[0]
        return remote(source, target, mat_send.at[index], mat_recv.at[index], (dom, 1))

    def pack_copy():
        return remote(pack_out, pack_in, pack_send, pack_recv, (dom, 0))

    def pick(row, place):
        return lanes(jnp.where(lane == place, row[:, :LANES], 0.0))

    def stage_copy():
        return remote(s_raw.at[1], halo_mat, stage_send, stage_recv, (dom, 0))

    def halo_copy(source):
        return remote(source, halo_mat, halo_send, halo_recv, (beyond, 1))

    def finish(sums, known_gamma, gamma_at, known_delta, delta_at, delta_next, gamma_inv, alpha_inv):
        even, odd = pick(sums, 0), pick(sums, 1)
        gamma = known_gamma + gamma_at * even
        delta = known_delta + delta_at * even + delta_next * odd
        beta = gamma * gamma_inv
        return beta, gamma / (delta - beta * gamma * alpha_inv)

    def put(sol, res, norm_list):
        out_ref[0:1] = sol
        out_ref[1:2] = res
        place_of = lax.broadcasted_iota(jnp.int32, (1, width), 1)
        norms = jnp.zeros((1, width), jnp.float32)
        for step in range(ITERS):
            norms = jnp.where(place_of == step, norm_list[step], norms)
        out_ref[2:3] = norms

    @pl.when(sub == 0)
    def _():
        lines[0] = rhs_ref[...]
        lines[1] = diag_ref[...]
        place = lax.broadcasted_iota(jnp.int32, (1, width), 1)
        for i in range(blocks):
            mask = jnp.zeros((1, width), jnp.float32)
            for j in range(blocks):
                mask = jnp.where(place // brow == j, pat_ref[i : i + 1, j : j + 1].astype(jnp.float32), mask)
            lines[2 + i] = mask
        pl.semaphore_wait(barrier, 1)
        line_copy().start()
        for index in range(3):
            mat_copy(index).start()
        if relays:
            @pl.when(wide)
            def _():
                pl.semaphore_wait(go, 1)

                @pl.when(far == 0)
                def _():
                    halo_copy(self_ref).start()

                @pl.when(far == 1)
                def _():
                    stage_copy().wait_recv()
                    halo_copy(halo_mat).start()

        line_copy().wait_send()
        for index in range(3):
            mat_copy(index).wait_send()
        if relays:
            @pl.when(wide)
            def _():
                halo_copy(halo_mat).wait_send()

        pack_copy().wait_recv()
        sol, resid, uvec, wvec, pvec, svec = [pack_in[index : index + 1] for index in range(6)]
        misc = pack_in[6:7]
        scalars = [pick(misc, place) for place in range(7 + ITERS)]
        every = red_buf.at[last_sums]
        pltpu.make_async_copy(every, every, r_recv.at[last_sums]).wait()
        beta, alpha = finish(jnp.sum(red_buf[last_sums], axis=0), *scalars[:7])
        put(sol + alpha * (uvec + beta * pvec), resid - alpha * (wvec + beta * svec), scalars[7:])

    @pl.when(sub == 1)
    def _():
        row_at, col_at = dom // n_col, dom % n_col
        pl.semaphore_signal(barrier, inc=1, device_id=(dom, 0), device_id_type=MESH)

        @pl.when(has_prev)
        def _():
            pl.semaphore_signal(barrier, inc=1, device_id=(dom - 1, 1), device_id_type=MESH)

        @pl.when(has_next)
        def _():
            pl.semaphore_signal(barrier, inc=1, device_id=(dom + 1, 1), device_id_type=MESH)

        def in_row(step):
            return (row_at * n_col + (col_at + step) % n_col, 1)

        def in_col(step):
            return (((row_at + step) % n_row) * n_col + col_at, 1)

        if n_col > 1:
            @pl.loop(1, n_col)
            def _(step):
                pl.semaphore_signal(barrier, inc=1, device_id=in_row(step), device_id_type=MESH)

        @pl.loop(1, n_row)
        def _(step):
            pl.semaphore_signal(barrier, inc=1, device_id=in_col(step), device_id_type=MESH)

        loads = [
            pltpu.make_async_copy(source, target, load_sem.at[index])
            for index, (source, target) in enumerate([
                (coup_ref, c_raw.at[1]), (self_ref, s_raw.at[1]), (pro_ref, p_raw.at[1]), (craw_ref, k_raw),
            ])
        ]
        for load in loads:
            load.start()

        @pl.when(dom == 0)
        def _():
            low_in[...] = jnp.zeros_like(low_in)
            edge_mat[0] = jnp.zeros_like(ft_mat)
            for k in range(1, 3 * ITERS):
                in_buf[k, 0] = jnp.zeros((1, width), jnp.float32)

        @pl.when(dom == n_dom - 1)
        def _():
            up_in[...] = jnp.zeros_like(up_in)
            for k in range(1, 3 * ITERS):
                in_buf[k, 1] = jnp.zeros((1, width), jnp.float32)

        def first_up():
            return remote(up_out, up_in, edge_send.at[0], edge_recv.at[0], (dom - 1, 1))

        def first_low():
            return remote(low_out, low_in, edge_send.at[1], edge_recv.at[1], (dom + 1, 1))

        def edge_matrix():
            return remote(ft_mat, edge_mat.at[0], edge_send.at[2], edge_recv.at[2], (dom + 1, 1))

        def to_side(k, side, place=None):
            source = out_buf.at[k if place is None else place, side]
            return remote(
                source, in_buf.at[k, 1 - side], out_send.at[k, side], in_recv.at[k, 1 - side], (dom + 2 * side - 1, 1)
            )

        def send(k, vec, wanted=(has_prev, has_next)):
            for side in range(2):
                out_buf[k, side] = vec[:, side * width : (side + 1) * width]

                @pl.when(wanted[side])
                def _():
                    to_side(k, side).start()

        has_near = jnp.where(near == 1, has_next, has_prev)
        has_far = jnp.where(near == 1, has_prev, has_next)
        order = ((near, has_near), (far, has_far))

        def receive(k, side, exists):
            @pl.when(exists)
            def _():
                landed = in_buf.at[k, side]
                pltpu.make_async_copy(landed, landed, in_recv.at[k, side]).wait()

            return in_buf[k, side]

        loads[0].wait()
        for i in range(blocks):
            for j in range(blocks):
                at = (slice(i * brow, (i + 1) * brow), slice(j * brow, (j + 1) * brow))
                edge_mat[1, at[0], at[1]] = c_raw[1, at[0], at[1]] * pat_ref[i : i + 1, j : j + 1].astype(jnp.float32)
        ft_mat[...] = edge_mat[1].T
        rhs_b, diag_b = rhs_ref[...], diag_ref[...]
        scale_b = OMEGA * (1.0 / diag_b)
        first_b = scale_b * rhs_b
        low_out[0] = down(edge_mat[1], upright(first_b))
        low_out[1] = scale_b

        pl.semaphore_wait(
            barrier,
            (n_row - 1) + (n_col - 1) + has_prev.astype(jnp.int32) + has_next.astype(jnp.int32),
        )

        @pl.when(has_next)
        def _():
            first_low().start()

        line_copy().wait_recv()
        rhs_a, diag_a = lines[0], lines[1]
        scale_a = OMEGA * (1.0 / diag_a)
        first_a = scale_a * rhs_a
        up_out[0] = first_a
        up_out[1] = scale_a

        @pl.when(has_prev)
        def _():
            first_up().start()

        @pl.when(has_next)
        def _():
            edge_matrix().start()

        if n_col > 1:
            @pl.loop(1, n_col)
            def _(step):
                pl.semaphore_signal(met, inc=1, device_id=in_row(step), device_id_type=MESH)

        rows = lax.broadcasted_iota(jnp.int32, (width, width), 0)
        cols = lax.broadcasted_iota(jnp.int32, (width, width), 1)
        same = rows == cols

        def put_self(index, diag):
            raw = s_raw[index]
            at = slice(index * width, (index + 1) * width)
            t_mat[index, :, at] = jnp.where(same, diag - diag * (1.0 / OMEGA), 0.5 * (raw + raw.T))

        for load in loads[1:]:
            load.wait()
        if relays:
            @pl.when(jnp.logical_and(wide, far == 1))
            def _():
                stage_copy().start()

            @pl.when(jnp.logical_not(wide))
            def _():
                halo_mat[...] = jnp.zeros_like(halo_mat)

        put_self(1, diag_b)
        pt_mat[1] = p_raw[1].T
        kinv = 1.0 / cdiag_ref[...]
        craw = k_raw[...]
        k_mat[...] = jnp.where(same, -kinv, (0.5 * (craw + craw.T)) * kinv * upright(kinv))

        rhs = jnp.concatenate([rhs_a, rhs_b], axis=1)
        scale = jnp.concatenate([scale_a, scale_b], axis=1)
        heavy = jnp.concatenate([diag_a, diag_b], axis=1) * (1.0 / OMEGA)
        minus = -upright(scale)

        mat_copy(0).wait_recv()
        put_self(0, diag_a)
        mat_copy(1).wait_recv()
        for i in range(blocks):
            at = slice(i * brow, (i + 1) * brow)
            block = c_raw[0, at, :] * lines[2 + i]
            t_mat[0, at, width:] = block
            t_mat[1, :, at] = block.T
        mat_copy(2).wait_recv()
        pt_mat[0] = p_raw[0].T

        def dot(left, right):
            return lanes(left * right)

        def start_sums(step, values):
            line = jnp.zeros((1, LANES), jnp.float32)
            for place, value in enumerate(values):
                line = jnp.where(lane == place, value, line)
            part_buf[step] = line
            red_buf[step, pl.ds(dom, 1)] = line[None]
            if step == first_sums:
                pl.semaphore_wait(known, n_row - 1)

            @pl.loop(0, n_dom - 1)
            def _(index):
                target = index + (index >= dom).astype(jnp.int32)
                for other in range(n_sub) if step == last_sums else (1,):
                    remote(
                        part_buf.at[step], red_buf.at[step, dom], r_send.at[step], r_recv.at[step],
                        (target, other),
                    ).start()

            if step == last_sums:
                remote(
                    part_buf.at[step], red_buf.at[step, dom], r_send.at[step], r_recv.at[step], (dom, 0)
                ).start()

        def end_sums(step):
            others = red_buf.at[step, pl.ds(0, n_dom - 1)]
            pltpu.make_async_copy(others, others, r_recv.at[step]).wait()
            return jnp.sum(red_buf[step], axis=0)

        def join(buffer):
            return jnp.concatenate([buffer[0], buffer[1]], axis=1)

        def edge_product(side):
            at = slice(side * coarse, (side + 1) * coarse)
            ke_mat[side] = product(k_mat[:, at], product(pt_mat[side], edge_mat[side]))

        def coarse_first(first):
            base_a, base_b = fold(t_mat[0], first), fold(t_mat[1], first)

            def from_prev():
                @pl.when(has_prev)
                def _():
                    first_low().wait_recv()

                rough_buf[0] = down(p_raw[0], lanes(base_a + embed(low_in[0])))

            def from_next():
                @pl.when(has_next)
                def _():
                    first_up().wait_recv()

                rough_buf[1] = down(p_raw[1], lanes(base_b + fold(edge_mat[1], up_in[0])))

            @pl.when(near == 0)
            def _():
                from_prev()
                from_next()

            @pl.when(near == 1)
            def _():
                from_next()
                from_prev()

            return lanes(fold(k_mat[...], join(rough_buf)))

        def coarse_later(k, first, halo):
            base = fold(kt_mat[...], first)
            for side, exists in order:
                row = receive(k, side, exists)
                if halo is not None and side is far:
                    row = jnp.where(wide, halo[0] - halo[1] * row, row)
                base = base + fold(ke_mat[side], row)
            return lanes(base)

        def side_of(side, vec):
            return jnp.where(side == 0, vec[:, :width], vec[:, width:])

        def short(side, vec, second):
            return fold(t_mat[side], second) - embed(side_of(side, vec))

        def across(vec, second):
            return jnp.concatenate([
                flat(lanes(fold(t_mat[side], second) - embed(vec[:, side * width : (side + 1) * width])))
                for side in range(2)
            ], axis=1)

        def round_of(t, vec, begin, held=None):
            first = scale * vec
            halo = None
            if held is not None:
                send(3 * t, first, (
                    jnp.logical_and(has_prev, dom % n_col != 0), jnp.logical_and(has_next, dom % n_col != n_col - 1)
                ))
            elif t:
                send(3 * t, first)
            begin()
            if held is not None:
                column, lost = held

                @pl.when(wide)
                def _():
                    halo_copy(halo_mat).wait_recv()

                far_scale = jnp.where(far == 0, low_in[1], up_in[1])
                far_diag = OMEGA / far_scale
                bare = jnp.where(same, 0.0, halo_mat[...])
                strong = 0.5 * (flat(lanes(fold(bare, lost))) + down(bare, upright(lost))) + far_diag * lost
                halo = in_buf[3, far] - far_scale * (down(edge_mat[far], column) - strong), far_scale
            if t == 1:
                edge_product(0)
            if t:
                turned = across(vec, first)
                etwo = coarse_later(3 * t, first, halo)
            else:
                etwo = coarse_first(first)
                rim_buf[0] = jnp.where(has_prev, low_in[1], 0.0)
                rim_buf[1] = jnp.where(has_next, up_in[1], 0.0)
            second = first + jnp.concatenate(
                [down(pt_mat[0], etwo[:coarse]), down(pt_mat[1], etwo[coarse:])], axis=1
            )
            send(3 * t + 1, second)
            if t:
                ghost = -scale * (turned + down(q_mat[...], etwo))
                send(3 * t + 2, ghost)
            base = {}
            for side, exists in order[::-1]:
                base[side is far] = short(side, vec, second)
                if not t:
                    out_buf[2, side] = -side_of(side, scale) * flat(lanes(base[side is far]))

                    @pl.when(exists)
                    def _():
                        to_side(2, side).start()

            upper = upright(second)
            if t == 0:
                @pl.when(has_next)
                def _():
                    edge_matrix().wait_send()

                if n_col > 1:
                    pl.semaphore_wait(met, n_col - 1)

                @pl.loop(1, n_row)
                def _(step):
                    pl.semaphore_signal(known, inc=1, device_id=in_col(step), device_id_type=MESH)

                if relays:
                    @pl.when(wide)
                    def _():
                        pl.semaphore_signal(go, inc=1, device_id=(dom, 0), device_id_type=MESH)

                for side in range(2):
                    q_mat[side * coarse : (side + 1) * coarse] = product(pt_mat[side], t_mat[side])
                kt_mat[...] = product(k_mat[...], q_mat[...])
                edge_product(1)
            else:
                for side in range(2):
                    side_buf[side] = rim_buf[side] * down(edge_mat[side], upper[side * width : (side + 1) * width])
            early = relays and t == 1
            if early:
                blank = jnp.zeros((1, width), jnp.float32)
                alone = jnp.concatenate(
                    [jnp.where(far == 0, ghost[:, :width], blank), jnp.where(far == 0, blank, ghost[:, width:])], axis=1
                )
                mine = flat(lanes(fold(t_mat[far], alone))) + side_of(far, heavy) * side_of(far, ghost)
            own = None
            for side, exists in order:
                if not t:
                    @pl.when(jnp.logical_and(side == 0, has_prev))
                    def _():
                        edge_matrix().wait_recv()

                ahead = receive(3 * t + 1, side, exists)
                joint = t and not (early and side is near)
                if joint:
                    other = receive(3 * t + 2, side, exists) - side_buf[side]
                total = base[side is far] + fold(edge_mat[side], ahead)
                column = jnp.where(side == 0, minus[:width], minus[width:]) * lanes(total)
                part = down(t_mat[side], column)
                if early and side is near:
                    @pl.when(wide)
                    def _():
                        out_buf[3 * ITERS, far] = side_of(far, part) + mine
                        to_side(3 * t + 3, far, 3 * ITERS).start()

                own = part if own is None else own + part
                turned = flat(column)
                if not t:
                    inner = jnp.where(side == 0, upper[:width], upper[width:])
                    lost = rim_buf[side] * down(edge_mat[side], inner)
                    other = receive(3 * t + 2, side, exists) - lost
                elif not joint:
                    other = receive(3 * t + 2, side, exists) - side_buf[side]
                crossed = flat(lanes(fold(edge_mat[side], other)))
                mid_buf[side] = turned
                end_buf[side] = crossed
            mvec = join(mid_buf)
            return mvec, own + heavy * mvec + join(end_buf), (column, side_buf[far]) if early else None

        dvecs, yvecs, held = [rhs], [], None
        eta, cross = [], {}

        def begin_of(t):
            def begin():
                if t:
                    eta.append(dot(dvecs[t], yvecs[t - 1]))
                    for k in range(t):
                        cross[k, t] = dot(dvecs[k], dvecs[t])
                    cross[t, t] = dot(dvecs[t], dvecs[t])
                else:
                    cross[0, 0] = dot(rhs, rhs)
                if t == last:
                    start_sums(first_sums, eta + [cross[place] for place in sorted(cross)])

            return begin

        for t in range(ITERS):
            yvec, bvec, held = round_of(t, dvecs[t], begin_of(t), held)
            yvecs.append(yvec)
            dvecs.append(dvecs[t] - bvec)
            if t < last:
                eta.append(dot(dvecs[t], yvec))
        start_sums(last_sums, [dot(dvecs[last], yvecs[last]), dot(dvecs[ITERS], yvecs[last])])

        sums = end_sums(first_sums)
        count = 2 * last
        eta = [pick(sums, place) for place in range(count)] + [0.0, 0.0]
        cross = {place: pick(sums, count + index) for index, place in enumerate(sorted(cross))}

        def pair(left, right):
            total = 0.0
            for i, one in enumerate(left):
                for j, other in enumerate(right):
                    total = plus(total, times(times(one, other), eta[i + j]))
            return total

        blank = [0.0] * (ITERS + 1)
        res = [1.0] + blank[1:]
        uco, wco = res, shift(res)
        pco, sco, qco, zco, sol = (blank,) * 5
        norm_list = []
        gamma_inv = alpha_inv = None
        for step in range(ITERS):
            norm = 0.0
            for i in range(step + 1):
                for j in range(step + 1):
                    norm = plus(norm, times(times(res[i], res[j]), cross[min(i, j), max(i, j)]))
            norm_list.append(norm)
            gamma, delta = pair(res[:ITERS], uco[:ITERS]), pair(wco, uco[:ITERS])
            if step == last:
                break
            if step == 0:
                beta, alpha = 0.0, gamma / delta
            else:
                beta = gamma * gamma_inv
                alpha = gamma / (delta - beta * gamma * alpha_inv)
            zco, qco = blend(beta, zco, shift(wco)), blend(beta, qco, wco)
            sco, pco = blend(beta, sco, wco), blend(beta, pco, uco)
            sol = blend(alpha, pco, sol)
            minus_alpha = -alpha
            res, uco, wco = blend(minus_alpha, sco, res), blend(minus_alpha, qco, uco), blend(minus_alpha, zco, wco)
            gamma_inv, alpha_inv = 1.0 / gamma, 1.0 / alpha
        final = [
            gamma, times(res[last], uco[last]),
            delta, plus(times(wco[last], uco[last]), times(wco[ITERS], uco[last - 1])), times(wco[ITERS], uco[last]),
            gamma_inv, alpha_inv,
        ]
        solution, uvec, pvec = [combine(row, yvecs) for row in (sol, uco, pco)]
        resid, wvec, svec = [combine(row, dvecs) for row in (res, wco, sco)]
        for index, vec in enumerate([solution, resid, uvec, wvec, pvec, svec]):
            pack_out[index : index + 1] = vec[:, :width]
        misc = jnp.zeros((1, LANES), jnp.float32)
        for place, value in enumerate(final + norm_list):
            misc = jnp.where(lane == place, value, misc)
        pack_out[6:7, :LANES] = misc
        pack_copy().start()
        pack_copy().wait_send()
        if relays:
            @pl.when(jnp.logical_and(wide, far == 1))
            def _():
                stage_copy().wait_send()

        @pl.when(has_prev)
        def _():
            first_up().wait_send()
            for k in range(1, 3 * ITERS):
                to_side(k, 0).wait_send()

        @pl.when(has_next)
        def _():
            first_low().wait_send()
            for k in range(1, 3 * ITERS):
                to_side(k, 1).wait_send()

        beta, alpha = finish(end_sums(last_sums), *final)
        put(
            (solution + alpha * (uvec + beta * pvec))[:, width:],
            (resid - alpha * (wvec + beta * svec))[:, width:],
            norm_list,
        )

        for step in (first_sums, last_sums):
            sent = red_buf.at[step, pl.ds(0, n_dom - 1)]
            pltpu.make_async_copy(sent, sent, r_send.at[step]).wait()
            if step == last_sums:
                every = red_buf.at[step]
                pltpu.make_async_copy(every, every, r_send.at[step]).wait()


def unpack(packed_ref, sol_ref, res_ref, norm_ref):
    sol_ref[...] = packed_ref[0]
    res_ref[...] = packed_ref[1]
    norm_ref[...] = packed_ref[2, : norm_ref.shape[0]]


def solution(mesh):
    n_dom, n_sub = mesh.shape["dom"], mesh.shape["sub"]

    def per_device(rhs, diagonal, self_raw, coupling, pattern, prolong, coarse_raw, coarse_diagonal):
        width = rhs.shape[0]
        coarse = prolong.shape[1]
        blocks = pattern.shape[0]
        steps = 3 * ITERS
        vmem = pl.BlockSpec(memory_space=pltpu.VMEM)
        hbm = pl.BlockSpec(memory_space=pl.ANY)
        single = jnp.float32
        dma = pltpu.SemaphoreType.DMA
        square = pltpu.VMEM((width, width), single)
        pair = pltpu.VMEM((2, 1, width), single)
        packed = pl.pallas_call(
            functools.partial(kernel, n_dom, n_sub),
            out_shape=jax.ShapeDtypeStruct((3, width), single),
            in_specs=[vmem, vmem, hbm, hbm, vmem, hbm, hbm, vmem],
            out_specs=vmem,
            scratch_shapes=[
                pltpu.VMEM((2 + blocks, 1, width), single),
                pltpu.VMEM((2, width, width), single),
                pltpu.VMEM((2, width, width), single),
                pltpu.VMEM((2, width, coarse), single),
                pltpu.VMEM((2 * coarse, 2 * coarse), single),
                pltpu.VMEM((2, width, width), single),
                square,
                pltpu.VMEM((2, width, 2 * width), single),
                pltpu.VMEM((2, coarse, width), single),
                pltpu.VMEM((2 * coarse, 2 * coarse), single),
                pltpu.VMEM((2 * coarse, 2 * width), single),
                pltpu.VMEM((2 * coarse, 2 * width), single),
                pltpu.VMEM((2, 2 * coarse, width), single),
                pair, pair, pair, pair,
                pltpu.VMEM((steps + 1, 2, 1, width), single),
                pltpu.VMEM((steps, 2, 1, width), single),
                pair, pair, pair, pair,
                pltpu.VMEM((2, 1, coarse), single),
                pltpu.VMEM((2, 1, LANES), single),
                pltpu.VMEM((2, n_dom, 1, LANES), single),
                pltpu.VMEM((8, width), single),
                pltpu.VMEM((8, width), single),
                square,
                pltpu.SemaphoreType.REGULAR, pltpu.SemaphoreType.REGULAR, pltpu.SemaphoreType.REGULAR,
                dma((4,)), dma, dma, dma((3,)), dma((3,)), dma((3,)), dma((3,)),
                dma((steps, 2)), dma((steps, 2)),
                dma((2,)), dma((2,)), dma, dma, dma, dma, dma, dma,
            ],
            compiler_params=pltpu.CompilerParams(
                collective_id=0, has_side_effects=True, vmem_limit_bytes=GRANT
            ),
        )(
            rhs.reshape(1, width), diagonal.reshape(1, width), self_raw, coupling, pattern,
            prolong, coarse_raw, coarse_diagonal.reshape(1, -1),
        )
        return pl.pallas_call(
            unpack,
            out_shape=(
                jax.ShapeDtypeStruct((width,), single),
                jax.ShapeDtypeStruct((width,), single),
                jax.ShapeDtypeStruct((ITERS,), single),
            ),
            in_specs=[vmem],
            out_specs=(vmem, vmem, vmem),
            compiler_params=pltpu.CompilerParams(vmem_limit_bytes=2**20),
        )(packed)

    line = P(("dom", "sub"))
    table = P(("dom", "sub"), None)
    return jax.shard_map(
        per_device,
        mesh=mesh,
        in_specs=(line, line, table, table, table, table, P("dom", None), P("dom")),
        out_specs=(line, line, P()),
        check_vma=False,
    )
```

```python
import functools

import jax
import jax.numpy as jnp
from jax import lax
from jax.experimental import pallas as pl
from jax.experimental.pallas import tpu as pltpu
from jax.sharding import PartitionSpec as P

ITERS = 3
OMEGA = 0.7
MESH = pl.DeviceIdType.MESH
LANES = 128
GRANT = 56_516_000


def factor(count):
    side = 1
    for trial in range(1, count + 1):
        if trial * trial <= count and count % trial == 0:
            side = trial
    return count // side, side


def fold(matrix, row):
    total = None
    for start in range(0, matrix.shape[1], LANES):
        part = matrix[:, start : start + LANES] * row[:, start : start + LANES]
        total = part if total is None else total + part
    return total


def lanes(block):
    return jnp.sum(block, axis=1, keepdims=True)


def down(matrix, column):
    return jnp.sum(matrix * column, axis=0, keepdims=True)


def times(left, right):
    if isinstance(left, float) and left in (0.0, 1.0):
        return right if left else 0.0
    if isinstance(right, float) and right in (0.0, 1.0):
        return left if right else 0.0
    return left * right


def plus(left, right):
    if isinstance(left, float) and left == 0.0:
        return right
    if isinstance(right, float) and right == 0.0:
        return left
    return left + right


def blend(scale, left, right):
    return [plus(one, times(scale, other)) for one, other in zip(right, left)]


def combine(weights, terms):
    total = 0.0
    for weight, term in zip(weights, terms):
        total = plus(total, times(weight, term))
    return total


def shift(row):
    return [plus(row[k], times(-1.0, row[k - 1])) if k else row[0] for k in range(len(row))]


def product(left, right):
    return jnp.dot(left, right, precision=lax.Precision.HIGHEST, preferred_element_type=jnp.float32)


def eye_of():
    rows = lax.broadcasted_iota(jnp.int32, (LANES, LANES), 0)
    cols = lax.broadcasted_iota(jnp.int32, (LANES, LANES), 1)
    return rows == cols


def embed(row):
    eye = eye_of()
    parts = [
        jnp.where(eye, row[:, start : start + LANES], 0.0) for start in range(0, row.shape[1], LANES)
    ]
    return jnp.concatenate(parts, axis=0)


def upright(row):
    return lanes(embed(row))


def flat(column):
    eye = eye_of()
    parts = [
        jnp.sum(jnp.where(eye, column[start : start + LANES], 0.0), axis=0, keepdims=True)
        for start in range(0, column.shape[0], LANES)
    ]
    return jnp.concatenate(parts, axis=1)


def kernel(
    n_dom, n_sub,
    rhs_ref, diag_ref, self_ref, coup_ref, pat_ref, pro_ref, craw_ref, cdiag_ref,
    out_ref,
    lines, s_raw, c_raw, p_raw, k_raw,
    edge_mat, ft_mat, t_mat, pt_mat, k_mat, q_mat, kt_mat, ke_mat,
    up_out, low_out, up_in, low_in, out_buf, in_buf, rim_buf, side_buf, mid_buf, end_buf, rough_buf,
    part_buf, red_buf, pack_out, pack_in, halo_mat,
    met, known, go, load_sem, line_send, line_recv, mat_send, mat_recv, edge_send, edge_recv,
    out_send, in_recv, r_send, r_recv, pack_send, pack_recv, halo_send, halo_recv, stage_send, stage_recv,
):
    dom, sub = lax.axis_index("dom"), lax.axis_index("sub")
    width = rhs_ref.shape[1]
    blocks = pat_ref.shape[0]
    brow = width // blocks
    coarse = pro_ref.shape[1]
    has_prev, has_next = dom > 0, dom < n_dom - 1
    n_row, n_col = factor(n_dom)
    barrier = pltpu.get_barrier_semaphore()
    first_sums, last_sums = range(2)
    last = ITERS - 1
    far = dom % 2
    near = 1 - far
    beyond = dom + 2 * far - 1
    wide = jnp.logical_or(jnp.logical_and(far == 0, has_prev), jnp.logical_and(far == 1, has_next))
    lane = lax.broadcasted_iota(jnp.int32, (1, LANES), 1)

    def remote(source, target, send, recv, device):
        return pltpu.make_async_remote_copy(
            source, target, send, recv, device_id=device, device_id_type=MESH
        )

    def line_copy():
        return remote(lines, lines, line_send, line_recv, (dom, 1))

    def mat_copy(index):
        source = (self_ref, coup_ref, pro_ref)[index]
        target = (s_raw, c_raw, p_raw)[index].at[0]
        return remote(source, target, mat_send.at[index], mat_recv.at[index], (dom, 1))

    def pack_copy():
        return remote(pack_out, pack_in, pack_send, pack_recv, (dom, 0))

    def pick(row, place):
        return lanes(jnp.where(lane == place, row[:, :LANES], 0.0))

    def stage_copy():
        return remote(s_raw.at[1], halo_mat, stage_send, stage_recv, (dom, 0))

    def halo_copy(source):
        return remote(source, halo_mat, halo_send, halo_recv, (beyond, 1))

    def finish(sums, known_gamma, gamma_at, known_delta, delta_at, delta_next, gamma_inv, alpha_inv):
        even, odd = pick(sums, 0), pick(sums, 1)
        gamma = known_gamma + gamma_at * even
        delta = known_delta + delta_at * even + delta_next * odd
        beta = gamma * gamma_inv
        return beta, gamma / (delta - beta * gamma * alpha_inv)

    def put(sol, res, norm_list):
        out_ref[0:1] = sol
        out_ref[1:2] = res
        place_of = lax.broadcasted_iota(jnp.int32, (1, width), 1)
        norms = jnp.zeros((1, width), jnp.float32)
        for step in range(ITERS):
            norms = jnp.where(place_of == step, norm_list[step], norms)
        out_ref[2:3] = norms

    @pl.when(sub == 0)
    def _():
        lines[0] = rhs_ref[...]
        lines[1] = diag_ref[...]
        place = lax.broadcasted_iota(jnp.int32, (1, width), 1)
        for i in range(blocks):
            mask = jnp.zeros((1, width), jnp.float32)
            for j in range(blocks):
                mask = jnp.where(place // brow == j, pat_ref[i : i + 1, j : j + 1].astype(jnp.float32), mask)
            lines[2 + i] = mask
        pl.semaphore_wait(barrier, 1)
        line_copy().start()
        for index in range(3):
            mat_copy(index).start()
        @pl.when(wide)
        def _():
            pl.semaphore_wait(go, 1)

            @pl.when(far == 0)
            def _():
                halo_copy(self_ref).start()

            @pl.when(far == 1)
            def _():
                stage_copy().wait_recv()
                halo_copy(halo_mat).start()

        line_copy().wait_send()
        for index in range(3):
            mat_copy(index).wait_send()
        @pl.when(wide)
        def _():
            halo_copy(halo_mat).wait_send()

        pack_copy().wait_recv()
        sol, resid, uvec, wvec, pvec, svec = [pack_in[index : index + 1] for index in range(6)]
        misc = pack_in[6:7]
        scalars = [pick(misc, place) for place in range(7 + ITERS)]
        every = red_buf.at[last_sums]
        pltpu.make_async_copy(every, every, r_recv.at[last_sums]).wait()
        beta, alpha = finish(jnp.sum(red_buf[last_sums], axis=0), *scalars[:7])
        put(sol + alpha * (uvec + beta * pvec), resid - alpha * (wvec + beta * svec), scalars[7:])

    @pl.when(sub == 1)
    def _():
        row_at, col_at = dom // n_col, dom % n_col
        has_near = jnp.where(near == 1, has_next, has_prev)
        has_far = jnp.where(near == 1, has_prev, has_next)
        order = ((near, has_near), (far, has_far))

        for side, exists in order[::-1]:
            @pl.when(exists)
            def _():
                pl.semaphore_signal(barrier, inc=1, device_id=(dom + 2 * side - 1, 1), device_id_type=MESH)

        pl.semaphore_signal(barrier, inc=1, device_id=(dom, 0), device_id_type=MESH)

        def in_row(step):
            return (row_at * n_col + (col_at + step) % n_col, 1)

        def in_col(step):
            return (((row_at + step) % n_row) * n_col + col_at, 1)

        if n_col > 1:
            @pl.loop(1, n_col)
            def _(step):
                pl.semaphore_signal(barrier, inc=1, device_id=in_row(step), device_id_type=MESH)

        @pl.loop(1, n_row)
        def _(step):
            pl.semaphore_signal(barrier, inc=1, device_id=in_col(step), device_id_type=MESH)

        loads = [
            pltpu.make_async_copy(source, target, load_sem.at[index])
            for index, (source, target) in enumerate([
                (coup_ref, c_raw.at[1]), (self_ref, s_raw.at[1]), (pro_ref, p_raw.at[1]), (craw_ref, k_raw),
            ])
        ]
        for load in loads:
            load.start()

        @pl.when(dom == 0)
        def _():
            low_in[...] = jnp.zeros_like(low_in)
            edge_mat[0] = jnp.zeros_like(ft_mat)
            for k in range(1, 3 * ITERS):
                in_buf[0, k] = jnp.zeros((1, width), jnp.float32)

        @pl.when(dom == n_dom - 1)
        def _():
            up_in[...] = jnp.zeros_like(up_in)
            for k in range(1, 3 * ITERS):
                in_buf[1, k] = jnp.zeros((1, width), jnp.float32)

        def first_up():
            return remote(up_out, up_in, edge_send.at[0], edge_recv.at[0], (dom - 1, 1))

        def first_low():
            return remote(low_out, low_in, edge_send.at[1], edge_recv.at[1], (dom + 1, 1))

        def edge_matrix():
            return remote(ft_mat, edge_mat.at[0], edge_send.at[2], edge_recv.at[2], (dom + 1, 1))

        def to_side(k, side, count=1, place=None):
            source = out_buf.at[side, pl.ds(k if place is None else place, count)]
            target = in_buf.at[1 - side, pl.ds(k, count)]
            return remote(source, target, out_send.at[side, k], in_recv.at[1 - side, k], (dom + 2 * side - 1, 1))

        def send(k, vecs, ways):
            for index, vec in enumerate(vecs):
                for side in range(2):
                    out_buf[side, k + index] = vec[:, side * width : (side + 1) * width]
            for side, exists in ways:
                @pl.when(exists)
                def _():
                    to_side(k, side, len(vecs)).start()

        def receive(k, side, exists, count=1):
            @pl.when(exists)
            def _():
                landed = in_buf.at[side, pl.ds(k, count)]
                pltpu.make_async_copy(landed, landed, in_recv.at[side, k]).wait()

            return [in_buf[side, k + index] for index in range(count)]

        loads[0].wait()
        for i in range(blocks):
            for j in range(blocks):
                at = (slice(i * brow, (i + 1) * brow), slice(j * brow, (j + 1) * brow))
                edge_mat[1, at[0], at[1]] = c_raw[1, at[0], at[1]] * pat_ref[i : i + 1, j : j + 1].astype(jnp.float32)
        ft_mat[...] = edge_mat[1].T
        rhs_b, diag_b = rhs_ref[...], diag_ref[...]
        scale_b = OMEGA * (1.0 / diag_b)
        first_b = scale_b * rhs_b
        low_out[0] = down(edge_mat[1], upright(first_b))
        low_out[1] = scale_b

        pl.semaphore_wait(
            barrier,
            (n_row - 1) + (n_col - 1) + has_prev.astype(jnp.int32) + has_next.astype(jnp.int32),
        )

        @pl.when(has_next)
        def _():
            first_low().start()

        line_copy().wait_recv()
        rhs_a, diag_a = lines[0], lines[1]
        scale_a = OMEGA * (1.0 / diag_a)
        first_a = scale_a * rhs_a
        up_out[0] = first_a
        up_out[1] = scale_a

        @pl.when(has_prev)
        def _():
            first_up().start()

        @pl.when(has_next)
        def _():
            edge_matrix().start()

        if n_col > 1:
            @pl.loop(1, n_col)
            def _(step):
                pl.semaphore_signal(met, inc=1, device_id=in_row(step), device_id_type=MESH)

        rows = lax.broadcasted_iota(jnp.int32, (width, width), 0)
        cols = lax.broadcasted_iota(jnp.int32, (width, width), 1)
        same = rows == cols

        def put_self(index, diag):
            raw = s_raw[index]
            at = slice(index * width, (index + 1) * width)
            t_mat[index, :, at] = jnp.where(same, diag - diag * (1.0 / OMEGA), 0.5 * (raw + raw.T))

        for load in loads[1:]:
            load.wait()
        @pl.when(jnp.logical_and(wide, far == 1))
        def _():
            stage_copy().start()

        @pl.when(jnp.logical_not(wide))
        def _():
            halo_mat[...] = jnp.zeros_like(halo_mat)

        put_self(1, diag_b)
        pt_mat[1] = p_raw[1].T
        kinv = 1.0 / cdiag_ref[...]
        craw = k_raw[...]
        k_mat[...] = jnp.where(same, -kinv, (0.5 * (craw + craw.T)) * kinv * upright(kinv))

        rhs = jnp.concatenate([rhs_a, rhs_b], axis=1)
        scale = jnp.concatenate([scale_a, scale_b], axis=1)
        heavy = jnp.concatenate([diag_a, diag_b], axis=1) * (1.0 / OMEGA)
        minus = -upright(scale)

        mat_copy(0).wait_recv()
        put_self(0, diag_a)
        mat_copy(1).wait_recv()
        for i in range(blocks):
            at = slice(i * brow, (i + 1) * brow)
            block = c_raw[0, at, :] * lines[2 + i]
            t_mat[0, at, width:] = block
            t_mat[1, :, at] = block.T
        mat_copy(2).wait_recv()
        pt_mat[0] = p_raw[0].T

        def dot(left, right):
            return lanes(left * right)

        def start_sums(step, values):
            line = jnp.zeros((1, LANES), jnp.float32)
            for place, value in enumerate(values):
                line = jnp.where(lane == place, value, line)
            part_buf[step] = line
            red_buf[step, pl.ds(dom, 1)] = line[None]
            if step == first_sums:
                pl.semaphore_wait(known, n_row - 1)

            @pl.loop(0, n_dom - 1)
            def _(index):
                target = index + (index >= dom).astype(jnp.int32)
                for other in range(n_sub) if step == last_sums else (1,):
                    remote(
                        part_buf.at[step], red_buf.at[step, dom], r_send.at[step], r_recv.at[step],
                        (target, other),
                    ).start()

            if step == last_sums:
                remote(
                    part_buf.at[step], red_buf.at[step, dom], r_send.at[step], r_recv.at[step], (dom, 0)
                ).start()

        def end_sums(step):
            others = red_buf.at[step, pl.ds(0, n_dom - 1)]
            pltpu.make_async_copy(others, others, r_recv.at[step]).wait()
            return jnp.sum(red_buf[step], axis=0)

        def join(buffer):
            return jnp.concatenate([buffer[0], buffer[1]], axis=1)

        def edge_product(side):
            at = slice(side * coarse, (side + 1) * coarse)
            ke_mat[side] = product(k_mat[:, at], product(pt_mat[side], edge_mat[side]))

        def coarse_first(first):
            base_a, base_b = fold(t_mat[0], first), fold(t_mat[1], first)

            def from_prev():
                @pl.when(has_prev)
                def _():
                    first_low().wait_recv()

                rough_buf[0] = down(p_raw[0], lanes(base_a + embed(low_in[0])))

            def from_next():
                @pl.when(has_next)
                def _():
                    first_up().wait_recv()

                rough_buf[1] = down(p_raw[1], lanes(base_b + fold(edge_mat[1], up_in[0])))

            @pl.when(near == 0)
            def _():
                from_prev()
                from_next()

            @pl.when(near == 1)
            def _():
                from_next()
                from_prev()

            return lanes(fold(k_mat[...], join(rough_buf)))

        def coarse_later(k, first, halo):
            base = fold(kt_mat[...], first)
            for side, exists in order:
                row, = receive(k, side, exists)
                if halo is not None and side is far:
                    row = jnp.where(wide, halo[0] - halo[1] * row, row)
                base = base + fold(ke_mat[side], row)
            return lanes(base)

        def side_of(side, vec):
            return jnp.where(side == 0, vec[:, :width], vec[:, width:])

        def short(side, vec, second):
            return fold(t_mat[side], second) - embed(side_of(side, vec))

        def across(vec, second):
            return jnp.concatenate([
                flat(lanes(fold(t_mat[side], second) - embed(vec[:, side * width : (side + 1) * width])))
                for side in range(2)
            ], axis=1)

        def round_of(t, vec, begin, held=None):
            first = scale * vec
            halo = None
            if t:
                send(3 * t, [first], order[::-1] if held is None else order[:1])
            begin()
            if held is not None:
                column, lost = held

                @pl.when(wide)
                def _():
                    halo_copy(halo_mat).wait_recv()

                far_scale = jnp.where(far == 0, low_in[1], up_in[1])
                far_diag = OMEGA / far_scale
                bare = jnp.where(same, 0.0, halo_mat[...])
                strong = 0.5 * (flat(lanes(fold(bare, lost))) + down(bare, upright(lost))) + far_diag * lost
                halo = in_buf[far, 3] - far_scale * (down(edge_mat[far], column) - strong), far_scale
            if t == 1:
                edge_product(0)
            if t:
                turned = across(vec, first)
                etwo = coarse_later(3 * t, first, halo)
            else:
                etwo = coarse_first(first)
                rim_buf[0] = jnp.where(has_prev, low_in[1], 0.0)
                rim_buf[1] = jnp.where(has_next, up_in[1], 0.0)
            second = first + jnp.concatenate(
                [down(pt_mat[0], etwo[:coarse]), down(pt_mat[1], etwo[coarse:])], axis=1
            )
            if t:
                ghost = -scale * (turned + down(q_mat[...], etwo))
                send(3 * t + 1, [second, ghost], order[::-1])
            else:
                send(3 * t + 1, [second], order[::-1])
            base = {}
            for side, exists in order[::-1]:
                base[side is far] = short(side, vec, second)
                if not t:
                    out_buf[side, 2] = -side_of(side, scale) * flat(lanes(base[side is far]))

                    @pl.when(exists)
                    def _():
                        to_side(2, side).start()

            upper = upright(second)
            if t == 0:
                @pl.when(has_next)
                def _():
                    edge_matrix().wait_send()

                if n_col > 1:
                    pl.semaphore_wait(met, n_col - 1)

                @pl.loop(1, n_row)
                def _(step):
                    pl.semaphore_signal(known, inc=1, device_id=in_col(step), device_id_type=MESH)

                @pl.when(wide)
                def _():
                    pl.semaphore_signal(go, inc=1, device_id=(dom, 0), device_id_type=MESH)

                for side in range(2):
                    q_mat[side * coarse : (side + 1) * coarse] = product(pt_mat[side], t_mat[side])
                kt_mat[...] = product(k_mat[...], q_mat[...])
                edge_product(1)
            else:
                for side in range(2):
                    side_buf[side] = rim_buf[side] * down(edge_mat[side], upper[side * width : (side + 1) * width])
            early = t == 1
            if early:
                blank = jnp.zeros((1, width), jnp.float32)
                alone = jnp.concatenate(
                    [jnp.where(far == 0, ghost[:, :width], blank), jnp.where(far == 0, blank, ghost[:, width:])], axis=1
                )
                mine = flat(lanes(fold(t_mat[far], alone))) + side_of(far, heavy) * side_of(far, ghost)
            own = None
            for side, exists in order:
                if not t:
                    @pl.when(jnp.logical_and(side == 0, has_prev))
                    def _():
                        edge_matrix().wait_recv()

                if t:
                    ahead, other = receive(3 * t + 1, side, exists, 2)
                    other = other - side_buf[side]
                else:
                    ahead, = receive(3 * t + 1, side, exists)
                total = base[side is far] + fold(edge_mat[side], ahead)
                column = jnp.where(side == 0, minus[:width], minus[width:]) * lanes(total)
                part = down(t_mat[side], column)
                if early and side is near:
                    @pl.when(wide)
                    def _():
                        out_buf[far, 3 * ITERS] = side_of(far, part) + mine
                        to_side(3 * t + 3, far, 1, 3 * ITERS).start()

                own = part if own is None else own + part
                turned = flat(column)
                if not t:
                    inner = jnp.where(side == 0, upper[:width], upper[width:])
                    lost = rim_buf[side] * down(edge_mat[side], inner)
                    other = receive(3 * t + 2, side, exists)[0] - lost
                crossed = flat(lanes(fold(edge_mat[side], other)))
                mid_buf[side] = turned
                end_buf[side] = crossed
            mvec = join(mid_buf)
            return mvec, own + heavy * mvec + join(end_buf), (column, side_buf[far]) if early else None

        sent_slots = [(1, 1), (2, 1)] + [(3 * t + part, 1 + part) for t in range(1, ITERS) for part in range(2)]
        dvecs, yvecs, held = [rhs], [], None
        eta, cross = [], {}

        def begin_of(t):
            def begin():
                if t:
                    eta.append(dot(dvecs[t], yvecs[t - 1]))
                    for k in range(t):
                        cross[k, t] = dot(dvecs[k], dvecs[t])
                    cross[t, t] = dot(dvecs[t], dvecs[t])
                else:
                    cross[0, 0] = dot(rhs, rhs)
                if t == last:
                    start_sums(first_sums, eta + [cross[place] for place in sorted(cross)])

            return begin

        for t in range(ITERS):
            yvec, bvec, held = round_of(t, dvecs[t], begin_of(t), held)
            yvecs.append(yvec)
            dvecs.append(dvecs[t] - bvec)
            if t < last:
                eta.append(dot(dvecs[t], yvec))
        start_sums(last_sums, [dot(dvecs[last], yvecs[last]), dot(dvecs[ITERS], yvecs[last])])

        sums = end_sums(first_sums)
        count = 2 * last
        eta = [pick(sums, place) for place in range(count)] + [0.0, 0.0]
        cross = {place: pick(sums, count + index) for index, place in enumerate(sorted(cross))}

        def pair(left, right):
            total = 0.0
            for i, one in enumerate(left):
                for j, other in enumerate(right):
                    total = plus(total, times(times(one, other), eta[i + j]))
            return total

        blank = [0.0] * (ITERS + 1)
        res = [1.0] + blank[1:]
        uco, wco = res, shift(res)
        pco, sco, qco, zco, sol = (blank,) * 5
        norm_list = []
        gamma_inv = alpha_inv = None
        for step in range(ITERS):
            norm = 0.0
            for i in range(step + 1):
                for j in range(step + 1):
                    norm = plus(norm, times(times(res[i], res[j]), cross[min(i, j), max(i, j)]))
            norm_list.append(norm)
            gamma, delta = pair(res[:ITERS], uco[:ITERS]), pair(wco, uco[:ITERS])
            if step == last:
                break
            if step == 0:
                beta, alpha = 0.0, gamma / delta
            else:
                beta = gamma * gamma_inv
                alpha = gamma / (delta - beta * gamma * alpha_inv)
            zco, qco = blend(beta, zco, shift(wco)), blend(beta, qco, wco)
            sco, pco = blend(beta, sco, wco), blend(beta, pco, uco)
            sol = blend(alpha, pco, sol)
            minus_alpha = -alpha
            res, uco, wco = blend(minus_alpha, sco, res), blend(minus_alpha, qco, uco), blend(minus_alpha, zco, wco)
            gamma_inv, alpha_inv = 1.0 / gamma, 1.0 / alpha
        final = [
            gamma, times(res[last], uco[last]),
            delta, plus(times(wco[last], uco[last]), times(wco[ITERS], uco[last - 1])), times(wco[ITERS], uco[last]),
            gamma_inv, alpha_inv,
        ]
        solution, uvec, pvec = [combine(row, yvecs) for row in (sol, uco, pco)]
        resid, wvec, svec = [combine(row, dvecs) for row in (res, wco, sco)]
        for index, vec in enumerate([solution, resid, uvec, wvec, pvec, svec]):
            pack_out[index : index + 1] = vec[:, :width]
        misc = jnp.zeros((1, LANES), jnp.float32)
        for place, value in enumerate(final + norm_list):
            misc = jnp.where(lane == place, value, misc)
        pack_out[6:7, :LANES] = misc
        pack_copy().start()
        pack_copy().wait_send()
        @pl.when(jnp.logical_and(wide, far == 1))
        def _():
            stage_copy().wait_send()

        @pl.when(has_prev)
        def _():
            first_up().wait_send()
            for k, count in sent_slots:
                to_side(k, 0, count).wait_send()

        @pl.when(has_next)
        def _():
            first_low().wait_send()
            for k, count in sent_slots:
                to_side(k, 1, count).wait_send()

        beta, alpha = finish(end_sums(last_sums), *final)
        put(
            (solution + alpha * (uvec + beta * pvec))[:, width:],
            (resid - alpha * (wvec + beta * svec))[:, width:],
            norm_list,
        )

        for step in (first_sums, last_sums):
            sent = red_buf.at[step, pl.ds(0, n_dom - 1)]
            pltpu.make_async_copy(sent, sent, r_send.at[step]).wait()
            if step == last_sums:
                every = red_buf.at[step]
                pltpu.make_async_copy(every, every, r_send.at[step]).wait()


def unpack(packed_ref, sol_ref, res_ref, norm_ref):
    sol_ref[...] = packed_ref[0]
    res_ref[...] = packed_ref[1]
    norm_ref[...] = packed_ref[2, : norm_ref.shape[0]]


def solution(mesh):
    n_dom, n_sub = mesh.shape["dom"], mesh.shape["sub"]

    def per_device(rhs, diagonal, self_raw, coupling, pattern, prolong, coarse_raw, coarse_diagonal):
        width = rhs.shape[0]
        coarse = prolong.shape[1]
        blocks = pattern.shape[0]
        steps = 3 * ITERS
        vmem = pl.BlockSpec(memory_space=pltpu.VMEM)
        hbm = pl.BlockSpec(memory_space=pl.ANY)
        single = jnp.float32
        dma = pltpu.SemaphoreType.DMA
        square = pltpu.VMEM((width, width), single)
        pair = pltpu.VMEM((2, 1, width), single)
        packed = pl.pallas_call(
            functools.partial(kernel, n_dom, n_sub),
            out_shape=jax.ShapeDtypeStruct((3, width), single),
            in_specs=[vmem, vmem, hbm, hbm, vmem, hbm, hbm, vmem],
            out_specs=vmem,
            scratch_shapes=[
                pltpu.VMEM((2 + blocks, 1, width), single),
                pltpu.VMEM((2, width, width), single),
                pltpu.VMEM((2, width, width), single),
                pltpu.VMEM((2, width, coarse), single),
                pltpu.VMEM((2 * coarse, 2 * coarse), single),
                pltpu.VMEM((2, width, width), single),
                square,
                pltpu.VMEM((2, width, 2 * width), single),
                pltpu.VMEM((2, coarse, width), single),
                pltpu.VMEM((2 * coarse, 2 * coarse), single),
                pltpu.VMEM((2 * coarse, 2 * width), single),
                pltpu.VMEM((2 * coarse, 2 * width), single),
                pltpu.VMEM((2, 2 * coarse, width), single),
                pair, pair, pair, pair,
                pltpu.VMEM((2, steps + 1, 1, width), single),
                pltpu.VMEM((2, steps, 1, width), single),
                pair, pair, pair, pair,
                pltpu.VMEM((2, 1, coarse), single),
                pltpu.VMEM((2, 1, LANES), single),
                pltpu.VMEM((2, n_dom, 1, LANES), single),
                pltpu.VMEM((8, width), single),
                pltpu.VMEM((8, width), single),
                square,
                pltpu.SemaphoreType.REGULAR, pltpu.SemaphoreType.REGULAR, pltpu.SemaphoreType.REGULAR,
                dma((4,)), dma, dma, dma((3,)), dma((3,)), dma((3,)), dma((3,)),
                dma((2, steps)), dma((2, steps)),
                dma((2,)), dma((2,)), dma, dma, dma, dma, dma, dma,
            ],
            compiler_params=pltpu.CompilerParams(
                collective_id=0, has_side_effects=True, vmem_limit_bytes=GRANT
            ),
        )(
            rhs.reshape(1, width), diagonal.reshape(1, width), self_raw, coupling, pattern,
            prolong, coarse_raw, coarse_diagonal.reshape(1, -1),
        )
        return pl.pallas_call(
            unpack,
            out_shape=(
                jax.ShapeDtypeStruct((width,), single),
                jax.ShapeDtypeStruct((width,), single),
                jax.ShapeDtypeStruct((ITERS,), single),
            ),
            in_specs=[vmem],
            out_specs=(vmem, vmem, vmem),
            compiler_params=pltpu.CompilerParams(vmem_limit_bytes=2**20),
        )(packed)

    line = P(("dom", "sub"))
    table = P(("dom", "sub"), None)
    return jax.shard_map(
        per_device,
        mesh=mesh,
        in_specs=(line, line, table, table, table, table, P("dom", None), P("dom")),
        out_specs=(line, line, P()),
        check_vma=False,
    )
```

```python
import functools

import jax
import jax.numpy as jnp
from jax import lax
from jax.experimental import pallas as pl
from jax.experimental.pallas import tpu as pltpu
from jax.sharding import PartitionSpec as P

ITERS = 3
OMEGA = 0.7
MESH = pl.DeviceIdType.MESH
LANES = 128
GRANT = 56_516_000


def factor(count):
    side = 1
    for trial in range(1, count + 1):
        if trial * trial <= count and count % trial == 0:
            side = trial
    return count // side, side


def fold(matrix, row):
    total = None
    for start in range(0, matrix.shape[1], LANES):
        part = matrix[:, start : start + LANES] * row[:, start : start + LANES]
        total = part if total is None else total + part
    return total


def lanes(block):
    return jnp.sum(block, axis=1, keepdims=True)


def down(matrix, column):
    return jnp.sum(matrix * column, axis=0, keepdims=True)


def times(left, right):
    if isinstance(left, float) and left in (0.0, 1.0):
        return right if left else 0.0
    if isinstance(right, float) and right in (0.0, 1.0):
        return left if right else 0.0
    return left * right


def plus(left, right):
    if isinstance(left, float) and left == 0.0:
        return right
    if isinstance(right, float) and right == 0.0:
        return left
    return left + right


def blend(scale, left, right):
    return [plus(one, times(scale, other)) for one, other in zip(right, left)]


def combine(weights, terms):
    total = 0.0
    for weight, term in zip(weights, terms):
        total = plus(total, times(weight, term))
    return total


def shift(row):
    return [plus(row[k], times(-1.0, row[k - 1])) if k else row[0] for k in range(len(row))]


def product(left, right):
    return jnp.dot(left, right, precision=lax.Precision.HIGHEST, preferred_element_type=jnp.float32)


def eye_of():
    rows = lax.broadcasted_iota(jnp.int32, (LANES, LANES), 0)
    cols = lax.broadcasted_iota(jnp.int32, (LANES, LANES), 1)
    return rows == cols


def embed(row):
    eye = eye_of()
    parts = [
        jnp.where(eye, row[:, start : start + LANES], 0.0) for start in range(0, row.shape[1], LANES)
    ]
    return jnp.concatenate(parts, axis=0)


def upright(row):
    return lanes(embed(row))


def flat(column):
    eye = eye_of()
    parts = [
        jnp.sum(jnp.where(eye, column[start : start + LANES], 0.0), axis=0, keepdims=True)
        for start in range(0, column.shape[0], LANES)
    ]
    return jnp.concatenate(parts, axis=1)


def kernel(
    n_dom, n_sub,
    rhs_ref, diag_ref, self_ref, coup_ref, pat_ref, pro_ref, craw_ref, cdiag_ref,
    out_ref,
    lines, s_raw, c_raw, p_raw, k_raw,
    edge_mat, ft_mat, t_mat, pt_mat, k_mat, q_mat, kt_mat, ke_mat,
    up_out, low_out, up_in, low_in, out_buf, in_buf, rim_buf, side_buf, mid_buf, end_buf, rough_buf,
    part_buf, red_buf, tail_buf, wide_buf, pack_out, pack_in, halo_mat,
    met, known, go, load_sem, line_send, line_recv, mat_send, mat_recv, edge_send, edge_recv,
    out_send, in_recv, r_send, r_recv, pack_send, pack_recv, halo_send, halo_recv, stage_send, stage_recv,
):
    dom, sub = lax.axis_index("dom"), lax.axis_index("sub")
    width = rhs_ref.shape[1]
    blocks = pat_ref.shape[0]
    brow = width // blocks
    coarse = pro_ref.shape[1]
    has_prev, has_next = dom > 0, dom < n_dom - 1
    n_row, n_col = factor(n_dom)
    barrier = pltpu.get_barrier_semaphore()
    first_sums, last_sums = range(2)
    last = ITERS - 1
    far = dom % 2
    near = 1 - far
    beyond = dom + 2 * far - 1
    wide = jnp.logical_or(jnp.logical_and(far == 0, has_prev), jnp.logical_and(far == 1, has_next))
    lane = lax.broadcasted_iota(jnp.int32, (1, LANES), 1)

    def remote(source, target, send, recv, device):
        return pltpu.make_async_remote_copy(
            source, target, send, recv, device_id=device, device_id_type=MESH
        )

    def line_copy():
        return remote(lines, lines, line_send, line_recv, (dom, 1))

    def mat_copy(index):
        source = (self_ref, coup_ref, pro_ref)[index]
        target = (s_raw, c_raw, p_raw)[index].at[0]
        return remote(source, target, mat_send.at[index], mat_recv.at[index], (dom, 1))

    def pack_copy():
        return remote(pack_out, pack_in, pack_send, pack_recv, (dom, 0))

    def pick(row, place):
        return lanes(jnp.where(lane == place, row[:, :LANES], 0.0))

    def stage_copy():
        return remote(s_raw.at[1], halo_mat, stage_send, stage_recv, (dom, 0))

    def halo_copy(source):
        return remote(source, halo_mat, halo_send, halo_recv, (beyond, 1))

    def finish(sums, known_gamma, gamma_at, known_delta, delta_at, delta_next, gamma_inv, alpha_inv):
        even, odd = lanes(sums[0]), lanes(sums[1])
        gamma = known_gamma + gamma_at * even
        delta = known_delta + delta_at * even + delta_next * odd
        beta = gamma * gamma_inv
        return beta, gamma / (delta - beta * gamma * alpha_inv)

    def put(sol, res, norm_list):
        out_ref[0:1] = sol
        out_ref[1:2] = res
        place_of = lax.broadcasted_iota(jnp.int32, (1, width), 1)
        norms = jnp.zeros((1, width), jnp.float32)
        for step in range(ITERS):
            norms = jnp.where(place_of == step, norm_list[step], norms)
        out_ref[2:3] = norms

    @pl.when(sub == 0)
    def _():
        lines[0] = rhs_ref[...]
        lines[1] = diag_ref[...]
        place = lax.broadcasted_iota(jnp.int32, (1, width), 1)
        for i in range(blocks):
            mask = jnp.zeros((1, width), jnp.float32)
            for j in range(blocks):
                mask = jnp.where(place // brow == j, pat_ref[i : i + 1, j : j + 1].astype(jnp.float32), mask)
            lines[2 + i] = mask
        pl.semaphore_wait(barrier, 1)
        line_copy().start()
        for index in range(3):
            mat_copy(index).start()
        @pl.when(wide)
        def _():
            pl.semaphore_wait(go, 1)

            @pl.when(far == 0)
            def _():
                halo_copy(self_ref).start()

            @pl.when(far == 1)
            def _():
                stage_copy().wait_recv()
                halo_copy(halo_mat).start()

        line_copy().wait_send()
        for index in range(3):
            mat_copy(index).wait_send()
        @pl.when(wide)
        def _():
            halo_copy(halo_mat).wait_send()

        pack_copy().wait_recv()
        sol, resid, uvec, wvec, pvec, svec = [pack_in[index : index + 1] for index in range(6)]
        misc = pack_in[6:7]
        scalars = [pick(misc, place) for place in range(7 + ITERS)]
        pltpu.make_async_copy(wide_buf, wide_buf, r_recv.at[last_sums]).wait()
        beta, alpha = finish(jnp.sum(wide_buf[...], axis=0), *scalars[:7])
        put(sol + alpha * (uvec + beta * pvec), resid - alpha * (wvec + beta * svec), scalars[7:])

    @pl.when(sub == 1)
    def _():
        row_at, col_at = dom // n_col, dom % n_col
        has_near = jnp.where(near == 1, has_next, has_prev)
        has_far = jnp.where(near == 1, has_prev, has_next)
        order = ((near, has_near), (far, has_far))

        for side, exists in order[::-1]:
            @pl.when(exists)
            def _():
                pl.semaphore_signal(barrier, inc=1, device_id=(dom + 2 * side - 1, 1), device_id_type=MESH)

        pl.semaphore_signal(barrier, inc=1, device_id=(dom, 0), device_id_type=MESH)

        def in_row(step):
            return (row_at * n_col + (col_at + step) % n_col, 1)

        def in_col(step):
            return (((row_at + step) % n_row) * n_col + col_at, 1)

        if n_col > 1:
            @pl.loop(1, n_col)
            def _(step):
                pl.semaphore_signal(barrier, inc=1, device_id=in_row(step), device_id_type=MESH)

        @pl.loop(1, n_row)
        def _(step):
            pl.semaphore_signal(barrier, inc=1, device_id=in_col(step), device_id_type=MESH)

        loads = [
            pltpu.make_async_copy(source, target, load_sem.at[index])
            for index, (source, target) in enumerate([
                (coup_ref, c_raw.at[1]), (self_ref, s_raw.at[1]), (pro_ref, p_raw.at[1]), (craw_ref, k_raw),
            ])
        ]
        for load in loads:
            load.start()

        @pl.when(dom == 0)
        def _():
            low_in[...] = jnp.zeros_like(low_in)
            edge_mat[0] = jnp.zeros_like(ft_mat)
            for k in range(1, 3 * ITERS):
                in_buf[0, k] = jnp.zeros((1, width), jnp.float32)

        @pl.when(dom == n_dom - 1)
        def _():
            up_in[...] = jnp.zeros_like(up_in)
            for k in range(1, 3 * ITERS):
                in_buf[1, k] = jnp.zeros((1, width), jnp.float32)

        def first_up():
            return remote(up_out, up_in, edge_send.at[0], edge_recv.at[0], (dom - 1, 1))

        def first_low():
            return remote(low_out, low_in, edge_send.at[1], edge_recv.at[1], (dom + 1, 1))

        def edge_matrix():
            return remote(ft_mat, edge_mat.at[0], edge_send.at[2], edge_recv.at[2], (dom + 1, 1))

        def to_side(k, side, count=1, place=None):
            source = out_buf.at[side, pl.ds(k if place is None else place, count)]
            target = in_buf.at[1 - side, pl.ds(k, count)]
            return remote(source, target, out_send.at[side, k], in_recv.at[1 - side, k], (dom + 2 * side - 1, 1))

        def send(k, vecs, ways):
            for index, vec in enumerate(vecs):
                for side in range(2):
                    out_buf[side, k + index] = vec[:, side * width : (side + 1) * width]
            for side, exists in ways:
                @pl.when(exists)
                def _():
                    to_side(k, side, len(vecs)).start()

        def receive(k, side, exists, count=1):
            @pl.when(exists)
            def _():
                landed = in_buf.at[side, pl.ds(k, count)]
                pltpu.make_async_copy(landed, landed, in_recv.at[side, k]).wait()

            return [in_buf[side, k + index] for index in range(count)]

        loads[0].wait()
        for i in range(blocks):
            for j in range(blocks):
                at = (slice(i * brow, (i + 1) * brow), slice(j * brow, (j + 1) * brow))
                edge_mat[1, at[0], at[1]] = c_raw[1, at[0], at[1]] * pat_ref[i : i + 1, j : j + 1].astype(jnp.float32)
        ft_mat[...] = edge_mat[1].T
        rhs_b, diag_b = rhs_ref[...], diag_ref[...]
        scale_b = OMEGA * (1.0 / diag_b)
        first_b = scale_b * rhs_b
        low_out[0] = down(edge_mat[1], upright(first_b))
        low_out[1] = scale_b

        pl.semaphore_wait(
            barrier,
            (n_row - 1) + (n_col - 1) + has_prev.astype(jnp.int32) + has_next.astype(jnp.int32),
        )

        @pl.when(has_next)
        def _():
            first_low().start()

        line_copy().wait_recv()
        rhs_a, diag_a = lines[0], lines[1]
        scale_a = OMEGA * (1.0 / diag_a)
        first_a = scale_a * rhs_a
        up_out[0] = first_a
        up_out[1] = scale_a

        @pl.when(has_prev)
        def _():
            first_up().start()

        @pl.when(has_next)
        def _():
            edge_matrix().start()

        if n_col > 1:
            @pl.loop(1, n_col)
            def _(step):
                pl.semaphore_signal(met, inc=1, device_id=in_row(step), device_id_type=MESH)

        rows = lax.broadcasted_iota(jnp.int32, (width, width), 0)
        cols = lax.broadcasted_iota(jnp.int32, (width, width), 1)
        same = rows == cols

        def put_self(index, diag):
            raw = s_raw[index]
            at = slice(index * width, (index + 1) * width)
            t_mat[index, :, at] = jnp.where(same, diag - diag * (1.0 / OMEGA), 0.5 * (raw + raw.T))

        for load in loads[1:]:
            load.wait()
        @pl.when(jnp.logical_and(wide, far == 1))
        def _():
            stage_copy().start()

        @pl.when(jnp.logical_not(wide))
        def _():
            halo_mat[...] = jnp.zeros_like(halo_mat)

        put_self(1, diag_b)
        pt_mat[1] = p_raw[1].T
        kinv = 1.0 / cdiag_ref[...]
        craw = k_raw[...]
        k_mat[...] = jnp.where(same, -kinv, (0.5 * (craw + craw.T)) * kinv * upright(kinv))

        rhs = jnp.concatenate([rhs_a, rhs_b], axis=1)
        scale = jnp.concatenate([scale_a, scale_b], axis=1)
        heavy = jnp.concatenate([diag_a, diag_b], axis=1) * (1.0 / OMEGA)
        minus = -upright(scale)

        mat_copy(0).wait_recv()
        put_self(0, diag_a)
        mat_copy(1).wait_recv()
        for i in range(blocks):
            at = slice(i * brow, (i + 1) * brow)
            block = c_raw[0, at, :] * lines[2 + i]
            t_mat[0, at, width:] = block
            t_mat[1, :, at] = block.T
        mat_copy(2).wait_recv()
        pt_mat[0] = p_raw[0].T

        def dot(left, right):
            return lanes(left * right)

        def strip(row):
            return sum(row[:, start : start + LANES] for start in range(0, row.shape[1], LANES))

        def each_other(run):
            @pl.loop(0, n_dom - 1)
            def _(index):
                run(index + (index >= dom).astype(jnp.int32))

        def start_sums(values):
            line = jnp.zeros((1, LANES), jnp.float32)
            for place, value in enumerate(values):
                line = jnp.where(lane == place, value, line)
            part_buf[...] = line
            red_buf[pl.ds(dom, 1)] = line[None]
            pl.semaphore_wait(known, n_row - 1)
            each_other(lambda target: remote(
                part_buf, red_buf.at[dom], r_send.at[first_sums], r_recv.at[first_sums], (target, 1)
            ).start())

        def last_copy(target, other):
            return remote(
                tail_buf, wide_buf.at[dom], r_send.at[last_sums], r_recv.at[last_sums], (target, other)
            )

        def start_last(rows):
            for index, row in enumerate(rows):
                tail_buf[index] = strip(row)
                wide_buf[dom, index] = strip(row)

            def run(target):
                for other in range(n_sub):
                    last_copy(target, other).start()

            each_other(run)
            last_copy(dom, 0).start()

        def end_sums(step):
            buffer = (red_buf, wide_buf)[step]
            others = buffer.at[pl.ds(0, n_dom - 1)]
            pltpu.make_async_copy(others, others, r_recv.at[step]).wait()
            return jnp.sum(buffer[...], axis=0)

        def join(buffer):
            return jnp.concatenate([buffer[0], buffer[1]], axis=1)

        def edge_product(side):
            at = slice(side * coarse, (side + 1) * coarse)
            ke_mat[side] = product(k_mat[:, at], product(pt_mat[side], edge_mat[side]))

        def coarse_first(first):
            base_a, base_b = fold(t_mat[0], first), fold(t_mat[1], first)

            def from_prev():
                @pl.when(has_prev)
                def _():
                    first_low().wait_recv()

                rough_buf[0] = down(p_raw[0], lanes(base_a + embed(low_in[0])))

            def from_next():
                @pl.when(has_next)
                def _():
                    first_up().wait_recv()

                rough_buf[1] = down(p_raw[1], lanes(base_b + fold(edge_mat[1], up_in[0])))

            @pl.when(near == 0)
            def _():
                from_prev()
                from_next()

            @pl.when(near == 1)
            def _():
                from_next()
                from_prev()

            return lanes(fold(k_mat[...], join(rough_buf)))

        def coarse_later(k, first, halo):
            base = fold(kt_mat[...], first)
            for side, exists in order:
                row, = receive(k, side, exists)
                if halo is not None and side is far:
                    row = jnp.where(wide, halo[0] - halo[1] * row, row)
                base = base + fold(ke_mat[side], row)
            return lanes(base)

        def side_of(side, vec):
            return jnp.where(side == 0, vec[:, :width], vec[:, width:])

        def short(side, vec, second):
            return fold(t_mat[side], second) - embed(side_of(side, vec))

        def across(vec, second):
            return jnp.concatenate([
                flat(lanes(fold(t_mat[side], second) - embed(vec[:, side * width : (side + 1) * width])))
                for side in range(2)
            ], axis=1)

        def round_of(t, vec, begin, held=None):
            first = scale * vec
            halo = None
            if t:
                send(3 * t, [first], order[::-1] if held is None else order[:1])
            begin()
            if held is not None:
                column, lost = held

                @pl.when(wide)
                def _():
                    halo_copy(halo_mat).wait_recv()

                far_scale = jnp.where(far == 0, low_in[1], up_in[1])
                far_diag = OMEGA / far_scale
                bare = jnp.where(same, 0.0, halo_mat[...])
                strong = 0.5 * (flat(lanes(fold(bare, lost))) + down(bare, upright(lost))) + far_diag * lost
                halo = in_buf[far, 3] - far_scale * (down(edge_mat[far], column) - strong), far_scale
            if t == 1:
                edge_product(0)
            if t:
                turned = across(vec, first)
                etwo = coarse_later(3 * t, first, halo)
            else:
                etwo = coarse_first(first)
                rim_buf[0] = jnp.where(has_prev, low_in[1], 0.0)
                rim_buf[1] = jnp.where(has_next, up_in[1], 0.0)
            second = first + jnp.concatenate(
                [down(pt_mat[0], etwo[:coarse]), down(pt_mat[1], etwo[coarse:])], axis=1
            )
            if t:
                ghost = -scale * (turned + down(q_mat[...], etwo))
                send(3 * t + 1, [second, ghost], order[::-1])
            else:
                send(3 * t + 1, [second], order[::-1])
            base = {}
            for side, exists in order[::-1]:
                base[side is far] = short(side, vec, second)
                if not t:
                    out_buf[side, 2] = -side_of(side, scale) * flat(lanes(base[side is far]))

                    @pl.when(exists)
                    def _():
                        to_side(2, side).start()

            upper = upright(second)
            if t == 0:
                @pl.when(has_next)
                def _():
                    edge_matrix().wait_send()

                if n_col > 1:
                    pl.semaphore_wait(met, n_col - 1)

                @pl.loop(1, n_row)
                def _(step):
                    pl.semaphore_signal(known, inc=1, device_id=in_col(step), device_id_type=MESH)

                @pl.when(wide)
                def _():
                    pl.semaphore_signal(go, inc=1, device_id=(dom, 0), device_id_type=MESH)

                for side in range(2):
                    q_mat[side * coarse : (side + 1) * coarse] = product(pt_mat[side], t_mat[side])
                kt_mat[...] = product(k_mat[...], q_mat[...])
                edge_product(1)
            else:
                for side in range(2):
                    side_buf[side] = rim_buf[side] * down(edge_mat[side], upper[side * width : (side + 1) * width])
            early = t == 1
            if early:
                blank = jnp.zeros((1, width), jnp.float32)
                alone = jnp.concatenate(
                    [jnp.where(far == 0, ghost[:, :width], blank), jnp.where(far == 0, blank, ghost[:, width:])], axis=1
                )
                mine = flat(lanes(fold(t_mat[far], alone))) + side_of(far, heavy) * side_of(far, ghost)
            own = None
            for side, exists in order:
                if not t:
                    @pl.when(jnp.logical_and(side == 0, has_prev))
                    def _():
                        edge_matrix().wait_recv()

                if t:
                    ahead, other = receive(3 * t + 1, side, exists, 2)
                    other = other - side_buf[side]
                else:
                    ahead, = receive(3 * t + 1, side, exists)
                total = base[side is far] + fold(edge_mat[side], ahead)
                column = jnp.where(side == 0, minus[:width], minus[width:]) * lanes(total)
                part = down(t_mat[side], column)
                if early and side is near:
                    @pl.when(wide)
                    def _():
                        out_buf[far, 3 * ITERS] = side_of(far, part) + mine
                        to_side(3 * t + 3, far, 1, 3 * ITERS).start()

                own = part if own is None else own + part
                turned = flat(column)
                if not t:
                    inner = jnp.where(side == 0, upper[:width], upper[width:])
                    lost = rim_buf[side] * down(edge_mat[side], inner)
                    other = receive(3 * t + 2, side, exists)[0] - lost
                crossed = flat(lanes(fold(edge_mat[side], other)))
                mid_buf[side] = turned
                end_buf[side] = crossed
            mvec = join(mid_buf)
            return mvec, own + heavy * mvec + join(end_buf), (column, side_buf[far]) if early else None

        sent_slots = [(1, 1), (2, 1)] + [(3 * t + part, 1 + part) for t in range(1, ITERS) for part in range(2)]
        dvecs, yvecs, held = [rhs], [], None
        eta, cross = [], {}

        def begin_of(t):
            def begin():
                if t:
                    eta.append(dot(dvecs[t], yvecs[t - 1]))
                    for k in range(t):
                        cross[k, t] = dot(dvecs[k], dvecs[t])
                    cross[t, t] = dot(dvecs[t], dvecs[t])
                else:
                    cross[0, 0] = dot(rhs, rhs)
                if t == last:
                    start_sums(eta + [cross[place] for place in sorted(cross)])

            return begin

        for t in range(ITERS):
            yvec, bvec, held = round_of(t, dvecs[t], begin_of(t), held)
            yvecs.append(yvec)
            dvecs.append(dvecs[t] - bvec)
            if t < last:
                eta.append(dot(dvecs[t], yvec))
        start_last([dvecs[last] * yvecs[last], dvecs[ITERS] * yvecs[last]])

        sums = end_sums(first_sums)
        count = 2 * last
        eta = [pick(sums, place) for place in range(count)] + [0.0, 0.0]
        cross = {place: pick(sums, count + index) for index, place in enumerate(sorted(cross))}

        def pair(left, right):
            total = 0.0
            for i, one in enumerate(left):
                for j, other in enumerate(right):
                    total = plus(total, times(times(one, other), eta[i + j]))
            return total

        blank = [0.0] * (ITERS + 1)
        res = [1.0] + blank[1:]
        uco, wco = res, shift(res)
        pco, sco, qco, zco, sol = (blank,) * 5
        norm_list = []
        gamma_inv = alpha_inv = None
        for step in range(ITERS):
            norm = 0.0
            for i in range(step + 1):
                for j in range(step + 1):
                    norm = plus(norm, times(times(res[i], res[j]), cross[min(i, j), max(i, j)]))
            norm_list.append(norm)
            gamma, delta = pair(res[:ITERS], uco[:ITERS]), pair(wco, uco[:ITERS])
            if step == last:
                break
            if step == 0:
                beta, alpha = 0.0, gamma / delta
            else:
                beta = gamma * gamma_inv
                alpha = gamma / (delta - beta * gamma * alpha_inv)
            zco, qco = blend(beta, zco, shift(wco)), blend(beta, qco, wco)
            sco, pco = blend(beta, sco, wco), blend(beta, pco, uco)
            sol = blend(alpha, pco, sol)
            minus_alpha = -alpha
            res, uco, wco = blend(minus_alpha, sco, res), blend(minus_alpha, qco, uco), blend(minus_alpha, zco, wco)
            gamma_inv, alpha_inv = 1.0 / gamma, 1.0 / alpha
        final = [
            gamma, times(res[last], uco[last]),
            delta, plus(times(wco[last], uco[last]), times(wco[ITERS], uco[last - 1])), times(wco[ITERS], uco[last]),
            gamma_inv, alpha_inv,
        ]
        solution, uvec, pvec = [combine(row, yvecs) for row in (sol, uco, pco)]
        resid, wvec, svec = [combine(row, dvecs) for row in (res, wco, sco)]
        for index, vec in enumerate([solution, resid, uvec, wvec, pvec, svec]):
            pack_out[index : index + 1] = vec[:, :width]
        misc = jnp.zeros((1, LANES), jnp.float32)
        for place, value in enumerate(final + norm_list):
            misc = jnp.where(lane == place, value, misc)
        pack_out[6:7, :LANES] = misc
        pack_copy().start()
        pack_copy().wait_send()
        @pl.when(jnp.logical_and(wide, far == 1))
        def _():
            stage_copy().wait_send()

        @pl.when(has_prev)
        def _():
            first_up().wait_send()
            for k, count in sent_slots:
                to_side(k, 0, count).wait_send()

        @pl.when(has_next)
        def _():
            first_low().wait_send()
            for k, count in sent_slots:
                to_side(k, 1, count).wait_send()

        beta, alpha = finish(end_sums(last_sums), *final)
        put(
            (solution + alpha * (uvec + beta * pvec))[:, width:],
            (resid - alpha * (wvec + beta * svec))[:, width:],
            norm_list,
        )

        for step, buffer in ((first_sums, red_buf), (last_sums, wide_buf)):
            sent = buffer.at[pl.ds(0, n_dom - 1)]
            pltpu.make_async_copy(sent, sent, r_send.at[step]).wait()
        pltpu.make_async_copy(wide_buf, wide_buf, r_send.at[last_sums]).wait()


def unpack(packed_ref, sol_ref, res_ref, norm_ref):
    sol_ref[...] = packed_ref[0]
    res_ref[...] = packed_ref[1]
    norm_ref[...] = packed_ref[2, : norm_ref.shape[0]]


def solution(mesh):
    n_dom, n_sub = mesh.shape["dom"], mesh.shape["sub"]

    def per_device(rhs, diagonal, self_raw, coupling, pattern, prolong, coarse_raw, coarse_diagonal):
        width = rhs.shape[0]
        coarse = prolong.shape[1]
        blocks = pattern.shape[0]
        steps = 3 * ITERS
        vmem = pl.BlockSpec(memory_space=pltpu.VMEM)
        hbm = pl.BlockSpec(memory_space=pl.ANY)
        single = jnp.float32
        dma = pltpu.SemaphoreType.DMA
        square = pltpu.VMEM((width, width), single)
        pair = pltpu.VMEM((2, 1, width), single)
        packed = pl.pallas_call(
            functools.partial(kernel, n_dom, n_sub),
            out_shape=jax.ShapeDtypeStruct((3, width), single),
            in_specs=[vmem, vmem, hbm, hbm, vmem, hbm, hbm, vmem],
            out_specs=vmem,
            scratch_shapes=[
                pltpu.VMEM((2 + blocks, 1, width), single),
                pltpu.VMEM((2, width, width), single),
                pltpu.VMEM((2, width, width), single),
                pltpu.VMEM((2, width, coarse), single),
                pltpu.VMEM((2 * coarse, 2 * coarse), single),
                pltpu.VMEM((2, width, width), single),
                square,
                pltpu.VMEM((2, width, 2 * width), single),
                pltpu.VMEM((2, coarse, width), single),
                pltpu.VMEM((2 * coarse, 2 * coarse), single),
                pltpu.VMEM((2 * coarse, 2 * width), single),
                pltpu.VMEM((2 * coarse, 2 * width), single),
                pltpu.VMEM((2, 2 * coarse, width), single),
                pair, pair, pair, pair,
                pltpu.VMEM((2, steps + 1, 1, width), single),
                pltpu.VMEM((2, steps, 1, width), single),
                pair, pair, pair, pair,
                pltpu.VMEM((2, 1, coarse), single),
                pltpu.VMEM((1, LANES), single),
                pltpu.VMEM((n_dom, 1, LANES), single),
                pltpu.VMEM((2, 1, LANES), single),
                pltpu.VMEM((n_dom, 2, 1, LANES), single),
                pltpu.VMEM((8, width), single),
                pltpu.VMEM((8, width), single),
                square,
                pltpu.SemaphoreType.REGULAR, pltpu.SemaphoreType.REGULAR, pltpu.SemaphoreType.REGULAR,
                dma((4,)), dma, dma, dma((3,)), dma((3,)), dma((3,)), dma((3,)),
                dma((2, steps)), dma((2, steps)),
                dma((2,)), dma((2,)), dma, dma, dma, dma, dma, dma,
            ],
            compiler_params=pltpu.CompilerParams(
                collective_id=0, has_side_effects=True, vmem_limit_bytes=GRANT
            ),
        )(
            rhs.reshape(1, width), diagonal.reshape(1, width), self_raw, coupling, pattern,
            prolong, coarse_raw, coarse_diagonal.reshape(1, -1),
        )
        return pl.pallas_call(
            unpack,
            out_shape=(
                jax.ShapeDtypeStruct((width,), single),
                jax.ShapeDtypeStruct((width,), single),
                jax.ShapeDtypeStruct((ITERS,), single),
            ),
            in_specs=[vmem],
            out_specs=(vmem, vmem, vmem),
            compiler_params=pltpu.CompilerParams(vmem_limit_bytes=2**20),
        )(packed)

    line = P(("dom", "sub"))
    table = P(("dom", "sub"), None)
    return jax.shard_map(
        per_device,
        mesh=mesh,
        in_specs=(line, line, table, table, table, table, P("dom", None), P("dom")),
        out_specs=(line, line, P()),
        check_vma=False,
    )
```
